32 devices in a mesh: dp: 8 (over y, z), tp: 4 (over x, core).
Axes of the slice: x: 2, y: 2, z: 4, core: 2. Of those that a mesh axis runs over, the one named last changes fastest.
Arguments:
- x: bfloat16 [8, 2048, 512], P('dp', 'tp')
- dy: bfloat16 [8, 2048, 512], P('dp', 'tp')
- wq: bfloat16 [512, 2048], P('dp', 'tp')
- wk: bfloat16 [512, 2048], P('dp', 'tp')
- wv: bfloat16 [512, 2048], P('dp', 'tp')
- wo: bfloat16 [2048, 512], P(('tp', 'dp'))
- w_gate: bfloat16 [512, 8192], P('dp', 'tp')
- w_up: bfloat16 [512, 8192], P('dp', 'tp')
- w_down: bfloat16 [8192, 512], P(('tp', 'dp'))
Outputs:
- output 1: bfloat16 [8, 2048, 512], P('dp', 'tp')
- output 2: bfloat16 [512, 2048], P('dp', 'tp')
- output 3: bfloat16 [512, 2048], P('dp', 'tp')
- output 4: bfloat16 [512, 2048], P('dp', 'tp')
- output 5: bfloat16 [2048, 512], P(('tp', 'dp'))
- output 6: bfloat16 [512, 8192], P('dp', 'tp')
- output 7: bfloat16 [512, 8192], P('dp', 'tp')
- output 8: bfloat16 [8192, 512], P(('tp', 'dp'))
All inputs are finite; a program needn't handle non-finite values.
Results may differ from the reference program's by a relative error of at most 0.024.
Values are sent between devices in bfloat16 or wider.
A program may use at most 2 GiB of HBM per device.

```python
import jax
import jax.numpy as jnp
from jax import lax

SEQUENCES = 8
TOKENS = 2048
D = 512
HEADS = 16
KV_HEADS = 16
HEAD = 128
FF = 8192
THETA = 10000
NAMES = ("wq", "wk", "wv", "wo", "w_gate", "w_up", "w_down")
SHAPES = {
    "wq": (D, HEADS * HEAD),
    "wk": (D, KV_HEADS * HEAD),
    "wv": (D, KV_HEADS * HEAD),
    "wo": (HEADS * HEAD, D),
    "w_gate": (D, FF),
    "w_up": (D, FF),
    "w_down": (FF, D),
}


def bump(key, n, height):
    away = (jnp.arange(n, dtype=jnp.int32) - jax.random.randint(key, (), 0, n, jnp.int32)) % n
    return jnp.where(away < n // 8, height, 1.0)


def together(key, own, strength):
    shared = jax.random.normal(key, own.shape[1:], jnp.float32)
    return (own + strength * shared) * lax.rsqrt(1 + strength * strength)


def setup_inputs(seed: int = 0, part: int = 0) -> dict:
    kx, kdy, ka, kb, kz, kf, kh, kl, *kw = jax.random.split(jax.random.key(seed), 8 + len(NAMES))
    shape = (SEQUENCES, TOKENS, D)
    much_x, much_dy = jax.random.uniform(kz, (2,), jnp.float32, 0.0, 1.0)
    loud = 2.0 ** jax.random.uniform(jax.random.fold_in(kz, 1), (), jnp.float32, -1.0, 2.0)
    halves = 2.0 ** jax.random.uniform(kl, (2,), jnp.float32, -1.0, 1.0)
    times = {"wq": 1.0, "wk": 1.0, "wv": 2.0, "wo": halves[0], "w_gate": 1.0, "w_up": bump(kh, FF, 4.0), "w_down": halves[1]}
    x = together(ka, jax.random.normal(kx, shape, jnp.float32), much_x) * bump(kf, D, 4.0)
    dy = together(kb, jax.random.normal(kdy, shape, jnp.float32), much_dy)
    drawn = {"x": x.astype(jnp.bfloat16), "dy": (loud * dy * (SEQUENCES * TOKENS) ** -0.5).astype(jnp.bfloat16)}
    for key, name in zip(kw, NAMES, strict=True):
        drawn[name] = (jax.random.normal(key, SHAPES[name], jnp.float32) * SHAPES[name][0] ** -0.5 * times[name]).astype(jnp.bfloat16)
    return drawn


def matmul(a, w):
    return jnp.dot(a, w, preferred_element_type=jnp.float32).astype(jnp.bfloat16)


def normed(h):
    wide = h.astype(jnp.float32)
    scale = lax.rsqrt(jnp.mean(wide**2, -1, keepdims=True) + 1e-6)
    return (wide * scale).astype(jnp.bfloat16)


def turned(t, theta):
    half = t.shape[-1] // 2
    angle = jnp.arange(t.shape[0], dtype=jnp.float32)[:, None] * theta ** (-jnp.arange(half, dtype=jnp.float32) / half)
    cos, sin = jnp.cos(angle)[:, None], jnp.sin(angle)[:, None]
    a, b = t[..., :half].astype(jnp.float32), t[..., half:].astype(jnp.float32)
    return jnp.concatenate([a * cos - b * sin, b * cos + a * sin], -1).astype(jnp.bfloat16)


def seen_by(q, k, v):
    tokens, kv = q.shape[0], k.shape[1]
    q = q.reshape(tokens, kv, -1, q.shape[-1])
    scores = jnp.einsum("tgsd,ugd->gstu", q.astype(jnp.float32), k.astype(jnp.float32)) * q.shape[-1] ** -0.5
    place = jnp.arange(tokens)
    weights = jax.nn.softmax(jnp.where(place[:, None] >= place, scores, -jnp.inf), -1).astype(jnp.bfloat16)
    return jnp.einsum("gstu,ugd->tgsd", weights.astype(jnp.float32), v.astype(jnp.float32)).astype(jnp.bfloat16).reshape(tokens, -1)


def layer(h, w):
    a = normed(h)
    q, k = (turned(matmul(a, w[name]).reshape(h.shape[0], -1, HEAD), THETA) for name in ("wq", "wk"))
    h = h + matmul(seen_by(q, k, matmul(a, w["wv"]).reshape(h.shape[0], -1, HEAD)), w["wo"])
    b = normed(h)
    gate = jnp.dot(b, w["w_gate"], preferred_element_type=jnp.float32)
    up = jnp.dot(b, w["w_up"], preferred_element_type=jnp.float32)
    return h + matmul((jax.nn.silu(gate) * up).astype(jnp.bfloat16), w["w_down"])


def reference(x, dy, wq, wk, wv, wo, w_gate, w_up, w_down):
    weights = dict(zip(NAMES, (wq, wk, wv, wo, w_gate, w_up, w_down), strict=True))

    def take(so_far, sequence):
        h, by_y = sequence
        _, back = jax.vjp(lambda w, h: layer(h, w), weights, h)
        by_weights, by_h = back(by_y)
        return jax.tree.map(lambda total, term: total + term.astype(jnp.float32), so_far, by_weights), by_h

    none_yet = {name: jnp.zeros(w.shape, jnp.float32) for name, w in weights.items()}
    by_weights, by_x = lax.scan(take, none_yet, (x, dy))
    return (by_x, *(by_weights[name].astype(jnp.bfloat16) for name in NAMES))
```

```python
import functools

import jax
import jax.numpy as jnp
from jax import lax
from jax.experimental import pallas as pl
from jax.experimental.pallas import tpu as pltpu
from jax.sharding import PartitionSpec as P

HEADS, HEAD, THETA = 4, 128, 10000
HALF = HEAD // 2
B = 512
TOKENS, FF, WIDE = 2048, 2048, 1024
NEG, HIDDEN = -1e30, -2e30
LOG2E = 1.4426950408889634
SCALE = HEAD**-0.5
F32, BF = jnp.float32, jnp.bfloat16
MESH = pl.DeviceIdType.MESH
ROOM = 67043328
ANY = pl.BlockSpec(memory_space=pl.ANY)
INV = pl.BlockSpec(memory_space=pltpu.VMEM)
RIGHT, LEFT, Y, YL, YR, MOVES = 0, 3, 6, 7, 10, 13


def _dot(a, b, ca, cb):
    return lax.dot_general(a, b, (((ca,), (cb,)), ((), ())), preferred_element_type=F32)


def _mm(a, b):
    return _dot(a, b, 1, 0)


def _mt(a, b):
    return _dot(a, b, 1, 1)


def _tm(a, b):
    return _dot(a, b, 0, 0)


def _normed(wide):
    return wide * lax.rsqrt(jnp.mean(wide * wide, -1, keepdims=True) + 1e-6)


def _normed_bwd(wide, g):
    r = lax.rsqrt(jnp.mean(wide * wide, -1, keepdims=True) + 1e-6)
    return g * r - wide * (r * r * r * jnp.mean(g * wide, -1, keepdims=True))


def _round(t):
    return t.astype(BF).astype(F32)


def _block(i):
    return pl.ds(pl.multiple_of(i * B, B), B)


def _send(src, dst, ss, rs, where):
    return pltpu.make_async_remote_copy(src_ref=src, dst_ref=dst, send_sem=ss, recv_sem=rs, device_id=where, device_id_type=MESH)


class Place:
    def __init__(self):
        self.dp, self.tp = lax.axis_index("dp"), lax.axis_index("tp")
        self.z, self.y = lax.rem(self.dp, 4), lax.div(self.dp, 4)
        self.row = self.y * 4
        self.other_row = 4 - self.row
        self.across = lax.rem(self.tp + 2, 4)
        self.core = self.tp + 1 - 2 * lax.rem(self.tp, 2)
        self.diagonal = 3 - self.tp
        self.to_y = {"dp": self.other_row + self.z, "tp": self.tp}
        self.to_right = {"dp": self.dp + 1, "tp": self.tp}
        self.to_left = {"dp": self.dp - 1, "tp": self.tp}
        self.to_across = {"dp": self.dp, "tp": self.across}
        self.to_core = {"dp": self.dp, "tp": self.core}

    def meet(self, dp, tp):
        bar = pltpu.get_barrier_semaphore()
        tell = lambda where: pl.semaphore_signal(bar, inc=1, device_id=where, device_id_type=MESH)
        count = 0
        if tp:
            tell(self.to_across)
            tell(self.to_core)
            count += 2
        if dp:
            tell(self.to_y)
            count += 1

            @pl.when(self.z > 0)
            def _():
                tell(self.to_left)

            @pl.when(self.z < 3)
            def _():
                tell(self.to_right)

            count += 1 + lax.div(self.z * (3 - self.z) + 1, 2)

        pl.semaphore_wait(bar, count)


class TpGather:
    def __init__(self, at, src, out, ss, rs, ls):
        self.own = pltpu.make_async_copy(src, out.at[at.tp], ls)
        self.a = _send(src, out.at[at.tp], ss.at[0], rs.at[0], at.to_across)
        self.c = _send(src, out.at[at.tp], ss.at[1], rs.at[1], at.to_core)
        self.f = _send(out.at[at.across], out.at[at.across], ss.at[2], rs.at[2], at.to_core)

    def start(self):
        self.a.start()
        self.c.start()
        self.own.start()

    def middle(self):
        self.a.wait_recv()
        self.f.start()

    def finish(self):
        self.c.wait_recv()
        self.f.wait_recv()
        self.a.wait_send()
        self.c.wait_send()
        self.f.wait_send()
        self.own.wait()


class DpGather:
    def __init__(self, at, srcs, outs, ss, rs, ls):
        self.at, self.srcs, self.outs, self.ss, self.rs, self.ls = at, srcs, outs, ss, rs, ls

    def move(self, n, i, first, origin, where):
        to = self.outs[n].at[origin]
        return _send(self.srcs[n] if first else to, to, self.ss.at[n, i], self.rs.at[n, i], where)

    def lines(self, n, s):
        at, first = self.at, s == 0
        yield (self.move(n, RIGHT + s, first, at.dp - s, at.to_right), jnp.logical_and(at.z >= s, at.z < 3),
               self.move(n, RIGHT + s, False, at.dp - 1 - s, at.to_right), at.z > s)
        yield (self.move(n, LEFT + s, first, at.dp + s, at.to_left), jnp.logical_and(at.z + s <= 3, at.z > 0),
               self.move(n, LEFT + s, False, at.dp + 1 + s, at.to_left), at.z + s < 3)

    def sides(self, n, r):
        at = self.at
        if r == 0:
            yield self.move(n, Y, True, at.dp, at.to_y), at.z >= 0
        else:
            yield self.move(n, YL + r - 1, False, at.dp - r, at.to_y), at.z >= r
            yield self.move(n, YR + r - 1, False, at.dp + r, at.to_y), at.z + r <= 3

    def local(self, n):
        return pltpu.make_async_copy(self.srcs[n], self.outs[n].at[self.at.dp], self.ls.at[n])

    def launch(self, n, r):
        if r < 3:
            for out, sends, _, _ in self.lines(n, r):
                pl.when(sends)(out.start)
        for out, sends in self.sides(n, r):
            pl.when(sends)(out.start)
        if r == 0:
            self.local(n).start()

    def arrive(self, n, r):
        for _, _, got, comes in self.lines(n, r):
            pl.when(comes)(got.wait_recv)

    def close(self, n, r):
        if r < 3:
            for out, sends, _, _ in self.lines(n, r):
                pl.when(sends)(out.wait_send)
        for out, sends in self.sides(n, r):
            pl.when(sends)(out.wait)
        if r == 0:
            self.local(n).wait()

    def next(self, n, r):
        self.arrive(n, r - 1)
        self.launch(n, r)


ORDER = ((3, 2, 1, 0), (3, 0, 2, 1), (0, 3, 1, 2), (0, 1, 2, 3))


class DpReduce:
    def __init__(self, at, parts, scratch, ss, rs, ls):
        self.at, self.parts, self.ss, self.rs, self.ls = at, parts, ss, rs, ls
        self.scratch = scratch

    def local(self, n):
        return pltpu.make_async_copy(self.parts[n].at[pl.ds(self.at.row, 4)], self.scratch[n][0], self.ls.at[n])

    def across(self, n, d):
        return _send(self.parts[n].at[self.at.other_row + d], self.scratch[n][1].at[d], self.ss.at[n, d], self.rs.at[n, d], self.at.to_y)

    def go_right(self, n, s, d):
        i = 4 + s
        return _send(self.scratch[n][0].at[d], self.scratch[n][2].at[s], self.ss.at[n, i], self.rs.at[n, i], self.at.to_right)

    def go_left(self, n, s, d):
        i = 7 + s
        return _send(self.scratch[n][0].at[d], self.scratch[n][3].at[s], self.ss.at[n, i], self.rs.at[n, i], self.at.to_left)

    def each(self, body):
        for z in range(4):
            pl.when(self.at.z == z)(functools.partial(body, z))

    def start(self):
        for n in range(len(self.parts)):
            self.local(n).start()

        def go(z):
            for d in ORDER[z]:
                for n in range(len(self.parts)):
                    self.across(n, d).start()

        self.each(go)

    def ready(self):
        for n in range(len(self.parts)):
            self.local(n).wait()

    def total(self, n, z, d, s, left, right):
        mine, got_y, from_left, from_right = self.scratch[n]
        self.across(n, d).wait_recv()
        total = mine[d].astype(F32) + got_y[d].astype(F32)
        if left:
            self.go_right(n, s, z).wait_recv()
            total = total + from_left[s].astype(F32)
        if right:
            self.go_left(n, s, z).wait_recv()
            total = total + from_right[s].astype(F32)
        return total.astype(BF)

    def stage(self, n, s):
        def go(z):
            mine = self.scratch[n][0]
            if z <= s and z < 3:
                d = 3 - s + z
                mine[d] = self.total(n, z, d, s - 1, z > 0, False)
                self.go_right(n, s, d).start()
            if z + s >= 3 and z > 0:
                d = s - 3 + z
                mine[d] = self.total(n, z, d, s - 1, False, z < 3)
                self.go_left(n, s, d).start()

        self.each(go)

    def finish(self, outs):
        def go(z):
            for n, out in enumerate(outs):
                out[:] = self.total(n, z, z, 2, z > 0, z < 3)
                for d in range(4):
                    self.across(n, d).wait_send()
                for s in range(3):
                    if z <= s and z < 3:
                        self.go_right(n, s, z).wait_send()
                    if z + s >= 3 and z > 0:
                        self.go_left(n, s, z).wait_send()

        self.each(go)


def _reduce_scratch(shapes):
    return [pltpu.VMEM((k, *s), BF) for s in shapes for k in (4, 4, 3, 3)]


def _reduce_sems(count):
    return _sems((count, 10), (count, 10), (count,))


class TpReduce:
    def __init__(self, at, to_c, from_c, to_a, from_a, near, ss, rs):
        self.at, self.to_c, self.from_c, self.to_a, self.from_a, self.near = at, to_c, from_c, to_a, from_a, near
        self.c = [_send(to_c.at[i], from_c.at[i], ss.at[i], rs.at[i], at.to_core) for i in range(2)]
        self.a = _send(to_a, from_a, ss.at[2], rs.at[2], at.to_across)

    def block(self, k):
        x, core = lax.div(self.at.tp, 2), lax.rem(self.at.tp, 2)
        other_x, other_core = 1 - lax.div(k, 2), 1 - lax.rem(k, 2)
        return 2 * (x + (1 - 2 * x) * other_x) + core + (1 - 2 * core) * other_core

    def add(self, k, term):
        for i in range(2):

            @pl.when(k == 2 * i)
            def _():
                self.to_c[i] = term.astype(BF)
                self.c[i].start()

        @pl.when(k == 1)
        def _():
            self.c[0].wait_recv()
            self.to_a[:] = (term + self.from_c[0].astype(F32)).astype(BF)
            self.a.start()

        @pl.when(k == 3)
        def _():
            self.c[1].wait_recv()
            self.near[:] = term + self.from_c[1].astype(F32)

    def total(self):
        self.a.wait()
        for c in self.c:
            c.wait_send()
        return self.near[:] + self.from_a[:].astype(F32)


def _tp_scratch():
    one, two = (B, B), (2, B, B)
    return [pltpu.VMEM(two, BF), pltpu.VMEM(two, BF), pltpu.VMEM(one, BF), pltpu.VMEM(one, BF), pltpu.VMEM(one, F32), *_sems((3,), (3,))]


def _sems(*shapes):
    return [pltpu.SemaphoreType.DMA(s) for s in shapes]


def _shape(shape, dtype=BF):
    return jax.ShapeDtypeStruct(shape, dtype)


BLOCK, STATES = _shape((B, B)), _shape((4, B, B))
PER_HEAD = _shape((HEADS, TOKENS, HEAD))


def _comm(kernel, name, number, ins, outs, out_specs, scratch, in_specs, aliases={}):
    return pl.pallas_call(
        kernel, name=name, out_shape=outs, in_specs=in_specs, out_specs=out_specs, scratch_shapes=scratch, input_output_aliases=aliases,
        compiler_params=pltpu.CompilerParams(collective_id=number, has_side_effects=True, vmem_limit_bytes=ROOM),
    )(*ins)


def _gather(x, dy, wq, wk, wv, wo):
    def kernel(x_ref, dy_ref, wq_ref, wk_ref, wv_ref, wo_ref, a_out, dy_out, wa_out, cos_ref, sin_ref, a_s, wa_s, ts, tr, tl, ds, dr, dl):
        at = Place()
        for i, w in enumerate((wq_ref, wk_ref, wv_ref, wo_ref)):
            wa_s[i] = w[:]
        a_s[:] = _normed(x_ref[:].astype(F32)).astype(BF)
        at.meet(True, True)
        weights = DpGather(at, [wa_s], [wa_out], ds, dr, dl)
        states = [TpGather(at, s, o, ts.at[n], tr.at[n], tl.at[n]) for n, (s, o) in enumerate(((a_s, a_out), (dy_ref, dy_out)))]
        weights.launch(0, 0)
        for s in states:
            s.start()

        def table(i, _):
            rows = 256
            here = pl.ds(pl.multiple_of(i * rows, rows), rows)
            lane = lax.broadcasted_iota(jnp.int32, (rows, HEAD), 1)
            token = (lax.broadcasted_iota(jnp.int32, (rows, HEAD), 0) + i * rows).astype(F32)
            low = lane < HALF
            angle = token * jnp.exp((jnp.where(low, lane, lane - HALF).astype(F32)) * (-jnp.log(jnp.float32(THETA)) / HALF))
            cos_ref[here, :] = jnp.cos(angle)
            sine = jnp.sin(angle)
            sin_ref[here, :] = jnp.where(low, -sine, sine)

        lax.fori_loop(0, TOKENS // 256, table, None)
        weights.next(0, 1)
        states[0].middle()
        weights.next(0, 2)
        weights.next(0, 3)
        states[1].middle()
        for s in states:
            s.finish()
        for r in range(4):
            weights.close(0, r)

    outs = [STATES, STATES, _shape((8, HEADS, *wq.shape))] + [_shape((TOKENS, HEAD), F32)] * 2
    scratch = [pltpu.VMEM((B, B), BF), pltpu.VMEM((HEADS, *wq.shape), BF), *_sems((2, 3), (2, 3), (2,), (1, MOVES), (1, MOVES), (1,))]
    return _comm(kernel, "gather", 0, (x, dy, wq, wk, wv, wo), outs, [ANY] * 3 + [INV] * 2, scratch, [INV] * 6)


def _turn(t, cos, sin):
    return t * cos + pltpu.roll(t, HALF, 1) * sin


def _gap(shape):
    return lax.broadcasted_iota(jnp.int32, shape, 1) - lax.broadcasted_iota(jnp.int32, shape, 0)


def _heads(t):
    return [t[:, h * HEAD : (h + 1) * HEAD] for h in range(HEADS)]


def _front(a, wa, cos, sin, wd, wg):
    e = SCALE * LOG2E

    def kernel(a_ref, wa_ref, cos_ref, sin_ref, wd_ref, wg_ref, q_ref, k_ref, v_ref, o_ref, lse_ref, d_out, g_out, top_s, mix_s, gap_s, ds, dr, dl):
        at = Place()
        at.meet(True, False)
        weights = DpGather(at, [wd_ref, wg_ref], [d_out, g_out], ds, dr, dl)
        weights.launch(0, 0)
        weights.launch(1, 0)
        gap_s[:] = _gap((B, B))

        def tile(t, _):
            here = _block(t)
            c, s = cos_ref[here, :], sin_ref[here, :]
            for i, ref in enumerate((q_ref, k_ref, v_ref)):
                all_heads = _mm(a_ref[t], wa_ref[:, i].reshape(B, B)).astype(BF)
                for h, one in enumerate(_heads(all_heads)):
                    ref[h, here, :] = one if ref is v_ref else _turn(one.astype(F32), c, s).astype(BF)
            top_s[:] = jnp.full_like(top_s, NEG)
            mix_s[:] = jnp.zeros_like(mix_s)
            ones = jnp.ones((8, B), BF)
            pl.when(t == 2)(lambda: weights.next(0, 1))
            pl.when(t == 3)(lambda: weights.next(0, 2))

            def block(j, masked):
                keys = _block(j)
                scores = [_mt(k_ref[h, keys, :], q_ref[h, here, :]) for h in range(HEADS)]
                weigh, keep = [], []
                for h, sc in enumerate(scores):
                    if masked:
                        sc = jnp.where(gap_s[:] >= 0, sc, HIDDEN)
                    one = slice(h, h + 1)
                    old = top_s[one, :]
                    top = jnp.maximum(old, sc.max(axis=0, keepdims=True))
                    top_s[one, :] = top
                    weigh.append(jnp.exp2((sc - top) * e).astype(BF))
                    keep.append(jnp.exp2((old - top) * e))
                for h in range(HEADS):
                    values = jnp.concatenate([v_ref[h, keys, :].T, ones], axis=0)
                    mix_s[h] = mix_s[h] * keep[h] + _mm(values, weigh[h])

            def whole(j, _):
                pl.when(jnp.logical_and(t == 2, j == 1))(lambda: weights.next(1, 1))
                block(j, False)

            lax.fori_loop(0, t, whole, None)
            pl.when(t == 3)(lambda: weights.next(0, 3))
            block(t, True)
            for h in range(HEADS):
                one = slice(h, h + 1)
                total = mix_s[h, HEAD : HEAD + 1, :]
                o_ref[h, here, :] = (mix_s[h, :HEAD, :] * (1 / total)).T.astype(BF)
                lse_ref[one, here] = top_s[one, :] * SCALE + jnp.log(total)

        lax.fori_loop(0, TOKENS // B, tile, None)
        weights.arrive(1, 1)
        for r in range(4):
            weights.close(0, r)
        for r in range(2):
            weights.close(1, r)

    outs = [PER_HEAD] * 4 + [_shape((HEADS, TOKENS), F32), _shape((8, *wd.shape)), _shape((8, *wg.shape))]
    scratch = [pltpu.VMEM((HEADS, B), F32), pltpu.VMEM((HEADS, HEAD + 8, B), F32), pltpu.VMEM((B, B), jnp.int32), *_sems((2, MOVES), (2, MOVES), (2,))]
    return _comm(kernel, "front", 1, (a, wa, cos, sin, wd, wg), outs, [INV] * 5 + [ANY] * 2, scratch, [INV] * 6)


def _mix(heads, wa, x, wg, wu, g):
    def kernel(heads_ref, wa_ref, x_ref, wg_ref, wu_ref, _, h_ref, b_out, g_out, u_out, b_s, *rest):
        *reduce, gs, gr, gl, ds, dr, dl = rest
        at = Place()
        at.meet(True, True)
        weights = DpGather(at, [wg_ref, wu_ref], [g_out, u_out], ds, dr, dl)
        weights.launch(0, 2)
        weights.launch(1, 0)
        sums = TpReduce(at, *reduce)
        wo = wa_ref[:, 3].reshape(B, B)
        for k in range(4):
            rows = _block(sums.block(k))
            sums.add(k, _mm(jnp.concatenate([heads_ref[h, rows, :] for h in range(HEADS)], axis=1), wo))
        weights.next(0, 3)
        weights.next(1, 1)
        h = (x_ref[:].astype(F32) + _round(sums.total())).astype(BF)
        h_ref[:] = h
        b_s[:] = _normed(h.astype(F32)).astype(BF)
        out = TpGather(at, b_s, b_out, gs, gr, gl)
        out.start()
        weights.next(1, 2)
        weights.next(1, 3)
        out.middle()
        out.finish()
        weights.close(0, 2)
        weights.close(0, 3)
        for r in range(4):
            weights.close(1, r)

    scratch = [pltpu.VMEM((B, B), BF), *_tp_scratch(), *_sems((3,), (3,), (), (2, MOVES), (2, MOVES), (2,))]
    return _comm(kernel, "mix", 2, (heads, wa, x, wg, wu, g), [BLOCK, STATES, _shape(g.shape), _shape(g.shape)], [INV] + [ANY] * 3, scratch,
                 [INV] * 5 + [ANY], {5: 2})


def _ffn(b, dy, g, u, d, h):
    chunks, per = FF // WIDE, WIDE // 256

    def kernel(b_ref, dy_ref, g_ref, u_ref, d_ref, h_ref, dh_ref, dg_ref, du_ref, dd_ref, dg_s, du_s, dd_s, wdt_s, wgut_s, db_s, *reduce):
        at = Place()
        at.meet(False, True)
        sums = TpReduce(at, *reduce)
        for acc in (dg_s, du_s, dd_s):
            acc[:] = jnp.zeros_like(acc)

        def columns(j):
            return pl.ds(pl.multiple_of(j * WIDE, WIDE), WIDE)

        def prepare(j, _):
            c = columns(j)
            wdt_s[:, c] = d_ref[pl.ds(j * per, per)].reshape(WIDE, B).T
            wgut_s[j, :WIDE] = g_ref[:, :, c].reshape(B, WIDE).T
            wgut_s[j, WIDE:] = u_ref[:, :, c].reshape(B, WIDE).T

        lax.fori_loop(0, chunks, prepare, None)

        def tile(k, _):
            t = sums.block(k)
            b, dy = b_ref[t], dy_ref[t]
            bt, dyt = b.T, dy.T
            db_s[:] = jnp.zeros_like(db_s)

            def hidden(j, _):
                c = columns(j)
                gate = _mm(b, g_ref[:, :, c].reshape(B, WIDE))
                up = _mm(b, u_ref[:, :, c].reshape(B, WIDE))
                dh = _round(_mm(dy, wdt_s[:, c]))
                sig = jax.nn.sigmoid(gate)
                act = gate * sig
                dup = (dh * act).astype(BF)
                dgate = (dh * up * (sig + act * (1 - sig))).astype(BF)
                db_s[:] += _mm(jnp.concatenate([dgate, dup], axis=1), wgut_s[j])
                dg_s[:, c] += _mm(bt, dgate)
                du_s[:, c] += _mm(bt, dup)
                dd_s[:, c] += _mm(dyt, (act * up).astype(BF))

            lax.fori_loop(0, chunks, hidden, None)
            sums.add(k, db_s[:])

        lax.fori_loop(0, TOKENS // B, tile, None)
        dg_ref[:] = dg_s[:].astype(BF)
        du_ref[:] = du_s[:].astype(BF)

        def store(j, _):
            c = columns(j)
            dd_ref[c, :] = dd_s[:, c].T.astype(BF)

        lax.fori_loop(0, chunks, store, None)
        back = _normed_bwd(h_ref[:].astype(F32), _round(sums.total()))
        dh_ref[:] = (dy_ref[at.tp].astype(F32) + _round(back)).astype(BF)

    acc = pltpu.VMEM((B, FF), F32)
    scratch = [acc, acc, acc, pltpu.VMEM((B, FF), BF), pltpu.VMEM((chunks, 2 * WIDE, B), BF), pltpu.VMEM((B, B), F32), *_tp_scratch()]
    return _comm(kernel, "ffn", 3, (b, dy, g, u, d, h), [BLOCK, _shape((B, FF)), _shape((B, FF)), _shape((FF, B))], [INV] * 4, scratch, [INV] * 6)


def _back(dh, a, wa, cos, sin, q, k, v, heads, lse, parts):
    e = SCALE * LOG2E
    count = len(parts)

    def kernel(dh_ref, a_ref, wa_ref, cos_ref, sin_ref, q_ref, k_ref, v_ref, o_ref, lse_ref, *refs):
        parts_ref, (da_ref, dwq_ref, dwk_ref, dwv_ref, dwo_ref, *refs) = refs[:count], refs[count:]
        outs, (dh_s, do_s, dq_s, dk_s, dv_s, gap_s, acc_s, gs, gr, gl, *refs) = refs[:count], refs[count:]
        scratch, (ds, dr, dl) = refs[: 4 * count], refs[4 * count :]
        at = Place()
        at.meet(True, True)
        sums = DpReduce(at, parts_ref, [scratch[4 * n : 4 * n + 4] for n in range(count)], ds, dr, dl)
        states = TpGather(at, dh_ref, dh_s, gs, gr, gl)
        states.start()
        sums.start()
        gap_s[:] = _gap((B, B))
        acc_s[:] = jnp.zeros_like(acc_s)
        dk_s[:] = jnp.zeros_like(dk_s)
        dv_s[:] = jnp.zeros_like(dv_s)
        states.middle()
        states.finish()
        sums.ready()

        def tile(i, _):
            t = 3 - i
            here = _block(t)

            @pl.when(i == 0)
            def _():
                sums.stage(0, 0)
                sums.stage(1, 0)

            @pl.when(i == 1)
            def _():
                sums.stage(0, 1)
                sums.stage(1, 1)

            @pl.when(i == 2)
            def _():
                sums.stage(0, 2)
                sums.stage(1, 2)

            pl.when(i == 3)(lambda: sums.stage(2, 2))
            dh = dh_s[t]
            mixed = [o_ref[h, here, :] for h in range(HEADS)]
            acc_s[3] += _tm(jnp.concatenate(mixed, axis=1), dh)
            do_s[:] = _mt(dh, wa_ref[:, 3].reshape(B, B)).astype(BF)
            dos = _heads(do_s)
            deltas = [(x.astype(F32) * y.astype(F32)).T.sum(axis=0, keepdims=True) for x, y in zip(dos, mixed)]
            lses = [lse_ref[h : h + 1, here] * LOG2E for h in range(HEADS)]
            dq_s[:] = jnp.zeros_like(dq_s)

            def block(j, masked):
                keys = _block(j)
                scores = [_mt(k_ref[h, keys, :], q_ref[h, here, :]) for h in range(HEADS)]
                dps = [_mt(v_ref[h, keys, :], do_s[:, h * HEAD : (h + 1) * HEAD]) for h in range(HEADS)]
                for h in range(HEADS):
                    p = jnp.exp2(scores[h] * e - lses[h])
                    if masked:
                        p = jnp.where(gap_s[:] >= 0, p, 0.0)
                    ds = (p * (dps[h] - deltas[h])).astype(BF)
                    dv_s[h, keys, :] += _mm(p.astype(BF), do_s[:, h * HEAD : (h + 1) * HEAD])
                    dk_s[h, keys, :] += _mm(ds, q_ref[h, here, :])
                    dq_s[h] += _mm(k_ref[h, keys, :].T, ds)

            def whole(j, _):
                for n in range(2):
                    pl.when(jnp.logical_and(i == n, j == 1))(lambda: sums.stage(2, n))
                block(j, False)

            lax.fori_loop(0, t, whole, None)
            block(t, True)
            c, s = cos_ref[here, :], -sin_ref[here, :]
            da = jnp.zeros((B, B), F32)
            for n, ref in enumerate((dq_s, dk_s, dv_s)):
                g = []
                for h in range(HEADS):
                    one = dq_s[h].T if ref is dq_s else ref[h, here, :]
                    g.append(one.astype(BF) if ref is dv_s else _turn(_round(one * SCALE), c, s).astype(BF))
                g = jnp.concatenate(g, axis=1)
                da += _mt(g, wa_ref[:, n].reshape(B, B))
                acc_s[n] += _tm(a_ref[t], g)
            da_ref[t] = da.astype(BF)

        lax.fori_loop(0, TOKENS // B, tile, None)
        for n, ref in enumerate((dwq_ref, dwk_ref, dwv_ref, dwo_ref)):
            ref[:] = acc_s[n].astype(BF)
        sums.finish(outs)

    blocks = [p.shape[1:] for p in parts]
    scratch = [pltpu.VMEM((4, B, B), BF), pltpu.VMEM((B, B), BF), pltpu.VMEM((HEADS, HEAD, B), F32), pltpu.VMEM(PER_HEAD.shape, F32), pltpu.VMEM(PER_HEAD.shape, F32),
               pltpu.VMEM((B, B), jnp.int32), pltpu.VMEM((4, B, B), F32), *_sems((3,), (3,), ()), *_reduce_scratch(blocks), *_reduce_sems(count)]
    return _comm(kernel, "back", 4, (dh, a, wa, cos, sin, q, k, v, heads, lse, *parts), [STATES, *[BLOCK] * 4, *map(_shape, blocks)], [INV] * (5 + count), scratch,
                 [INV] * 10 + [ANY] * count)


def _finish(da, x, dh, parts):
    count = len(parts)

    def kernel(da_ref, x_ref, dh_ref, *refs):
        parts_ref, (dx_ref, *refs) = refs[:count], refs[count:]
        outs, (*refs, ds, dr, dl) = refs[:count], refs[count:]
        tp = len(refs) - 4 * count
        reduce, scratch = refs[:tp], refs[tp:]
        at = Place()
        at.meet(True, True)
        weights = DpReduce(at, parts_ref, [scratch[4 * n : 4 * n + 4] for n in range(count)], ds, dr, dl)
        weights.start()
        sums = TpReduce(at, *reduce)
        for k in range(4):
            sums.add(k, da_ref[sums.block(k)].astype(F32))
        weights.ready()
        for s in range(2):
            for n in range(count):
                weights.stage(n, s)
        back = _normed_bwd(x_ref[:].astype(F32), _round(sums.total()))
        dx_ref[:] = (dh_ref[:].astype(F32) + _round(back)).astype(BF)
        for n in range(count):
            weights.stage(n, 2)
        weights.finish(outs)

    blocks = [p.shape[1:] for p in parts]
    scratch = [*_tp_scratch(), *_reduce_scratch(blocks), *_reduce_sems(count)]
    return _comm(kernel, "finish", 5, (da, x, dh, *parts), [BLOCK, *map(_shape, blocks)], [INV] * (1 + count), scratch, [INV] * 3 + [ANY] * count)


def _copies(arrays):
    count = len(arrays)

    def kernel(*refs):
        for a, b in zip(refs[:count], refs[count:]):
            b[:] = a[:]

    return pl.pallas_call(kernel, name="copies", out_shape=[_shape(a.shape) for a in arrays], in_specs=[INV] * count, out_specs=[INV] * count)(*arrays)


def solution(mesh):
    def step(x, dy, wq, wk, wv, wo, wg, wu, wd):
        x, dy = x[0], dy[0]
        a, all_dy, wa, cos, sin = _gather(x, dy, wq, wk, wv, wo)
        q, k, v, heads, lse, d, g = _front(a, wa, cos, sin, wd, wg)
        h, b, g, u = _mix(heads, wa, x, wg, wu, g)
        dh, *parts = _ffn(b, all_dy, g, u, d, h)
        split = lambda parts: [w.reshape(8, w.shape[0] // 8, w.shape[1]) for w in parts]
        da, *more = _back(dh, a, wa, cos, sin, q, k, v, heads, lse, split(parts))
        dx, *grads = _copies([*_finish(da, x, dh, split(more[:4])), *more[4:]])
        return (dx[None], *grads)

    states, by_columns, by_rows = P("dp", "tp", None), P("dp", "tp"), P(("tp", "dp"), None)
    weights = (by_columns, by_columns, by_columns, by_rows, by_columns, by_columns, by_rows)
    return jax.shard_map(step, mesh=mesh, in_specs=(states, states, *weights), out_specs=(states, *weights), check_vma=False)
```

```python
import functools

import jax
import jax.numpy as jnp
from jax import lax
from jax.experimental import pallas as pl
from jax.experimental.pallas import tpu as pltpu
from jax.sharding import PartitionSpec as P

HEADS, HEAD, THETA = 4, 128, 10000
HALF = HEAD // 2
B = 512
TOKENS, FF, WIDE = 2048, 2048, 1024
NEG, HIDDEN = -1e30, -2e30
LOG2E = 1.4426950408889634
SCALE = HEAD**-0.5
F32, BF = jnp.float32, jnp.bfloat16
MESH = pl.DeviceIdType.MESH
ROOM = 67043328
ANY = pl.BlockSpec(memory_space=pl.ANY)
INV = pl.BlockSpec(memory_space=pltpu.VMEM)
EARLY = 2
RIGHT, LEFT, Y, YL, YR, MOVES = 0, 3, 6, 7, 10, 13


def _dot(a, b, ca, cb):
    return lax.dot_general(a, b, (((ca,), (cb,)), ((), ())), preferred_element_type=F32)


def _mm(a, b):
    return _dot(a, b, 1, 0)


def _mt(a, b):
    return _dot(a, b, 1, 1)


def _tm(a, b):
    return _dot(a, b, 0, 0)


def _normed(wide):
    return wide * lax.rsqrt(jnp.mean(wide * wide, -1, keepdims=True) + 1e-6)


def _normed_bwd(wide, g):
    r = lax.rsqrt(jnp.mean(wide * wide, -1, keepdims=True) + 1e-6)
    return g * r - wide * (r * r * r * jnp.mean(g * wide, -1, keepdims=True))


def _round(t):
    return t.astype(BF).astype(F32)


def _block(i):
    return pl.ds(pl.multiple_of(i * B, B), B)


def _send(src, dst, ss, rs, where):
    return pltpu.make_async_remote_copy(src_ref=src, dst_ref=dst, send_sem=ss, recv_sem=rs, device_id=where, device_id_type=MESH)


class Place:
    def __init__(self):
        self.dp, self.tp = lax.axis_index("dp"), lax.axis_index("tp")
        self.z, self.y = lax.rem(self.dp, 4), lax.div(self.dp, 4)
        self.row = self.y * 4
        self.other_row = 4 - self.row
        self.across = lax.rem(self.tp + 2, 4)
        self.core = self.tp + 1 - 2 * lax.rem(self.tp, 2)
        self.diagonal = 3 - self.tp
        self.to_y = {"dp": self.other_row + self.z, "tp": self.tp}
        self.to_right = {"dp": self.dp + 1, "tp": self.tp}
        self.to_left = {"dp": self.dp - 1, "tp": self.tp}
        self.to_across = {"dp": self.dp, "tp": self.across}
        self.to_core = {"dp": self.dp, "tp": self.core}

    def meet(self, dp, tp):
        bar = pltpu.get_barrier_semaphore()
        tell = lambda where: pl.semaphore_signal(bar, inc=1, device_id=where, device_id_type=MESH)
        count = 0
        if tp:
            tell(self.to_across)
            tell(self.to_core)
            count += 2
        if dp:
            tell(self.to_y)
            count += 1

            @pl.when(self.z > 0)
            def _():
                tell(self.to_left)

            @pl.when(self.z < 3)
            def _():
                tell(self.to_right)

            count += 1 + lax.div(self.z * (3 - self.z) + 1, 2)

        pl.semaphore_wait(bar, count)


class TpGather:
    def __init__(self, at, src, out, ss, rs, ls):
        self.own = None if src is None else pltpu.make_async_copy(src, out.at[at.tp], ls)
        src = out.at[at.tp] if src is None else src
        self.a = _send(src, out.at[at.tp], ss.at[0], rs.at[0], at.to_across)
        self.c = _send(src, out.at[at.tp], ss.at[1], rs.at[1], at.to_core)
        self.f = _send(out.at[at.across], out.at[at.across], ss.at[2], rs.at[2], at.to_core)

    def start(self):
        self.a.start()
        self.c.start()
        if self.own is not None:
            self.own.start()

    def middle(self):
        self.a.wait_recv()
        self.f.start()

    def finish(self):
        self.c.wait_recv()
        self.f.wait_recv()
        self.a.wait_send()
        self.c.wait_send()
        self.f.wait_send()
        if self.own is not None:
            self.own.wait()


class DpGather:
    def __init__(self, at, srcs, outs, ss, rs, ls):
        self.at, self.srcs, self.outs, self.ss, self.rs, self.ls = at, srcs, outs, ss, rs, ls

    def move(self, n, i, first, origin, where):
        to = self.outs[n].at[origin]
        src = self.srcs[n] if first and self.srcs[n] is not None else to
        return _send(src, to, self.ss.at[n, i], self.rs.at[n, i], where)

    def lines(self, n, s):
        at, first = self.at, s == 0
        yield (self.move(n, RIGHT + s, first, at.dp - s, at.to_right), jnp.logical_and(at.z >= s, at.z < 3),
               self.move(n, RIGHT + s, False, at.dp - 1 - s, at.to_right), at.z > s)
        yield (self.move(n, LEFT + s, first, at.dp + s, at.to_left), jnp.logical_and(at.z + s <= 3, at.z > 0),
               self.move(n, LEFT + s, False, at.dp + 1 + s, at.to_left), at.z + s < 3)

    def sides(self, n, r):
        at = self.at
        if r == 0:
            yield self.move(n, Y, True, at.dp, at.to_y), at.z >= 0
        else:
            yield self.move(n, YL + r - 1, False, at.dp - r, at.to_y), at.z >= r
            yield self.move(n, YR + r - 1, False, at.dp + r, at.to_y), at.z + r <= 3

    def local(self, n):
        return pltpu.make_async_copy(self.srcs[n], self.outs[n].at[self.at.dp], self.ls.at[n])

    def launch(self, n, r):
        if r < 3:
            for out, sends, _, _ in self.lines(n, r):
                pl.when(sends)(out.start)
        for out, sends in self.sides(n, r):
            pl.when(sends)(out.start)
        if r == 0 and self.srcs[n] is not None:
            self.local(n).start()

    def arrive(self, n, r):
        for _, _, got, comes in self.lines(n, r):
            pl.when(comes)(got.wait_recv)

    def close(self, n, r):
        if r < 3:
            for out, sends, _, _ in self.lines(n, r):
                pl.when(sends)(out.wait_send)
        for out, sends in self.sides(n, r):
            pl.when(sends)(out.wait)
        if r == 0 and self.srcs[n] is not None:
            self.local(n).wait()

    def next(self, n, r):
        self.arrive(n, r - 1)
        self.launch(n, r)


ORDER = ((3, 2, 1, 0), (3, 0, 2, 1), (0, 3, 1, 2), (0, 1, 2, 3))


class DpReduce:
    def __init__(self, at, parts, scratch, ss, rs, ls, early=None):
        self.at, self.parts, self.ss, self.rs, self.ls = at, parts, ss, rs, ls
        self.scratch, self.early = scratch, early

    def local(self, n):
        return pltpu.make_async_copy(self.parts[n].at[pl.ds(self.at.row, 4)], self.scratch[n][0], self.ls.at[n])

    def across(self, n, d):
        return _send(self.parts[n].at[self.at.other_row + d], self.scratch[n][1].at[d], self.ss.at[n, d], self.rs.at[n, d], self.at.to_y)

    def go_right(self, n, s, d):
        i = 4 + s
        return _send(self.scratch[n][0].at[d], self.scratch[n][2].at[s], self.ss.at[n, i], self.rs.at[n, i], self.at.to_right)

    def go_left(self, n, s, d):
        i = 7 + s
        return _send(self.scratch[n][0].at[d], self.scratch[n][3].at[s], self.ss.at[n, i], self.rs.at[n, i], self.at.to_left)

    def came(self, n, i):
        return self.early is not None and n == 0 and i < EARLY

    def each(self, body):
        for z in range(4):
            pl.when(self.at.z == z)(functools.partial(body, z))

    def start(self):
        for n in range(len(self.parts)):
            self.local(n).start()

        def go(z):
            for i, d in enumerate(ORDER[z]):
                for n in range(len(self.parts)):
                    if self.came(n, i):
                        pltpu.make_async_copy(self.early.at[d], self.scratch[n][1].at[d], self.rs.at[n, d]).start()
                    else:
                        self.across(n, d).start()

        self.each(go)

    def ready(self):
        for n in range(len(self.parts)):
            self.local(n).wait()

    def total(self, n, z, d, s, left, right):
        mine, got_y, from_left, from_right = self.scratch[n]
        if self.came(n, ORDER[z].index(d)):
            pltpu.make_async_copy(self.early.at[d], got_y.at[d], self.rs.at[n, d]).wait()
        else:
            self.across(n, d).wait_recv()
        total = mine[d].astype(F32) + got_y[d].astype(F32)
        if left:
            self.go_right(n, s, z).wait_recv()
            total = total + from_left[s].astype(F32)
        if right:
            self.go_left(n, s, z).wait_recv()
            total = total + from_right[s].astype(F32)
        return total.astype(BF)

    def stage(self, n, s):
        def go(z):
            mine = self.scratch[n][0]
            if z <= s and z < 3:
                d = 3 - s + z
                mine[d] = self.total(n, z, d, s - 1, z > 0, False)
                self.go_right(n, s, d).start()
            if z + s >= 3 and z > 0:
                d = s - 3 + z
                mine[d] = self.total(n, z, d, s - 1, False, z < 3)
                self.go_left(n, s, d).start()

        self.each(go)

    def finish(self, outs):
        def go(z):
            for n, out in enumerate(outs):
                out[:] = self.total(n, z, z, 2, z > 0, z < 3)
                for i, d in enumerate(ORDER[z]):
                    if not self.came(n, i):
                        self.across(n, d).wait_send()
                for s in range(3):
                    if z <= s and z < 3:
                        self.go_right(n, s, z).wait_send()
                    if z + s >= 3 and z > 0:
                        self.go_left(n, s, z).wait_send()

        self.each(go)


def _reduce_scratch(shapes):
    return [pltpu.VMEM((k, *s), BF) for s in shapes for k in (4, 4, 3, 3)]


def _reduce_sems(count):
    return _sems((count, 10), (count, 10), (count,))


class TpReduce:
    def __init__(self, at, to_c, from_c, to_a, from_a, near, ss, rs):
        self.at, self.to_c, self.from_c, self.to_a, self.from_a, self.near = at, to_c, from_c, to_a, from_a, near
        self.c = [_send(to_c.at[i], from_c.at[i], ss.at[i], rs.at[i], at.to_core) for i in range(2)]
        self.a = _send(to_a, from_a, ss.at[2], rs.at[2], at.to_across)

    def block(self, k):
        x, core = lax.div(self.at.tp, 2), lax.rem(self.at.tp, 2)
        other_x, other_core = 1 - lax.div(k, 2), 1 - lax.rem(k, 2)
        return 2 * (x + (1 - 2 * x) * other_x) + core + (1 - 2 * core) * other_core

    def add(self, k, term):
        for i in range(2):

            @pl.when(k == 2 * i)
            def _():
                self.to_c[i] = term.astype(BF)
                self.c[i].start()

        @pl.when(k == 1)
        def _():
            self.c[0].wait_recv()
            self.to_a[:] = (term + self.from_c[0].astype(F32)).astype(BF)
            self.a.start()

        @pl.when(k == 3)
        def _():
            self.c[1].wait_recv()
            self.near[:] = term + self.from_c[1].astype(F32)

    def total(self):
        self.a.wait()
        for c in self.c:
            c.wait_send()
        return self.near[:] + self.from_a[:].astype(F32)


def _tp_scratch():
    one, two = (B, B), (2, B, B)
    return [pltpu.VMEM(two, BF), pltpu.VMEM(two, BF), pltpu.VMEM(one, BF), pltpu.VMEM(one, BF), pltpu.VMEM(one, F32), *_sems((3,), (3,))]


def _sems(*shapes):
    return [pltpu.SemaphoreType.DMA(s) for s in shapes]


def _shape(shape, dtype=BF):
    return jax.ShapeDtypeStruct(shape, dtype)


BLOCK, STATES = _shape((B, B)), _shape((4, B, B))
PER_HEAD = _shape((HEADS, TOKENS, HEAD))


def _comm(kernel, name, number, ins, outs, out_specs, scratch, in_specs, aliases={}):
    return pl.pallas_call(
        kernel, name=name, out_shape=outs, in_specs=in_specs, out_specs=out_specs, scratch_shapes=scratch, input_output_aliases=aliases,
        compiler_params=pltpu.CompilerParams(collective_id=number, has_side_effects=True, vmem_limit_bytes=ROOM),
    )(*ins)


def _turn(t, cos, sin):
    return t * cos + pltpu.roll(t, HALF, 1) * sin


def _gap(shape):
    return lax.broadcasted_iota(jnp.int32, shape, 1) - lax.broadcasted_iota(jnp.int32, shape, 0)


def _heads(t):
    return [t[:, h * HEAD : (h + 1) * HEAD] for h in range(HEADS)]


def _forward(x, dy, wq, wk, wv, wo, wg, wu, wd):
    e = SCALE * LOG2E

    def kernel(x_ref, dy_ref, wq_ref, wk_ref, wv_ref, wo_ref, wg_ref, wu_ref, wd_ref,
               h_ref, b_out, a_out, dy_out, wqkv_out, wo_out, g_out, u_out, d_out, q_out, k_out, v_out, o_out, lse_ref, cos_ref, sin_ref,
               a_s, b_s, wqkv_s, wo_s, q_ref, k_ref, v_ref, o_ref, top_s, mix_s, gap_s, ts, tr, tl, ds, dr, dl, ls, *reduce):
        at = Place()
        for i, w in enumerate((wq_ref, wk_ref, wv_ref)):
            wqkv_s[at.dp, i] = w[:]
        wo_s[at.dp] = wo_ref[:]
        a_s[at.tp] = _normed(x_ref[:].astype(F32)).astype(BF)
        at.meet(True, True)
        weights = DpGather(at, [None, None, wd_ref, wg_ref, wu_ref], [wqkv_s, wo_s, d_out, g_out, u_out], ds, dr, dl)
        qkv, last, down, gate, up = range(5)
        states = [TpGather(at, s, o, ts.at[n], tr.at[n], tl.at[n]) for n, (s, o) in enumerate(((None, a_s), (dy_ref, dy_out), (b_s, b_out)))]
        weights.launch(qkv, 0)
        weights.launch(last, 0)
        states[0].start()
        states[1].start()

        def table(i, _):
            rows = 256
            here = pl.ds(pl.multiple_of(i * rows, rows), rows)
            lane = lax.broadcasted_iota(jnp.int32, (rows, HEAD), 1)
            token = (lax.broadcasted_iota(jnp.int32, (rows, HEAD), 0) + i * rows).astype(F32)
            low = lane < HALF
            angle = token * jnp.exp((jnp.where(low, lane, lane - HALF).astype(F32)) * (-jnp.log(jnp.float32(THETA)) / HALF))
            cos_ref[here, :] = jnp.cos(angle)
            sine = jnp.sin(angle)
            sin_ref[here, :] = jnp.where(low, -sine, sine)

        lax.fori_loop(0, TOKENS // 256, table, None)
        gap_s[:] = _gap((B, B))
        for r in (1, 2):
            weights.next(qkv, r)
            weights.next(last, r)
        states[0].middle()
        weights.next(qkv, 3)
        weights.next(last, 3)
        weights.launch(down, 0)
        weights.launch(gate, 0)
        states[0].finish()
        for r in range(4):
            weights.close(qkv, r)

        def tile(t, _):
            here = _block(t)
            c, s = cos_ref[here, :], sin_ref[here, :]
            for i, ref in enumerate((q_ref, k_ref, v_ref)):
                all_heads = _mm(a_s[t], wqkv_s[:, i].reshape(B, B)).astype(BF)
                for h, one in enumerate(_heads(all_heads)):
                    ref[h, here, :] = one if ref is v_ref else _turn(one.astype(F32), c, s).astype(BF)
            top_s[:] = jnp.full_like(top_s, NEG)
            mix_s[:] = jnp.zeros_like(mix_s)
            ones = jnp.ones((8, B), BF)
            pl.when(t == 1)(lambda: states[1].middle())
            pl.when(t == 2)(lambda: weights.next(down, 1))
            pl.when(t == 3)(lambda: weights.next(down, 2))

            def block(j, masked):
                keys = _block(j)
                scores = [_mt(k_ref[h, keys, :], q_ref[h, here, :]) for h in range(HEADS)]
                weigh, keep = [], []
                for h, sc in enumerate(scores):
                    if masked:
                        sc = jnp.where(gap_s[:] >= 0, sc, HIDDEN)
                    one = slice(h, h + 1)
                    old = top_s[one, :]
                    top = jnp.maximum(old, sc.max(axis=0, keepdims=True))
                    top_s[one, :] = top
                    weigh.append(jnp.exp2((sc - top) * e).astype(BF))
                    keep.append(jnp.exp2((old - top) * e))
                for h in range(HEADS):
                    values = jnp.concatenate([v_ref[h, keys, :].T, ones], axis=0)
                    mix_s[h] = mix_s[h] * keep[h] + _mm(values, weigh[h])

            def whole(j, _):
                pl.when(jnp.logical_and(t == 2, j == 1))(lambda: weights.next(gate, 1))
                pl.when(jnp.logical_and(t == 3, j == 1))(lambda: weights.next(gate, 2))
                block(j, False)

            lax.fori_loop(0, t, whole, None)
            pl.when(t == 3)(lambda: weights.next(down, 3))
            block(t, True)
            for h in range(HEADS):
                one = slice(h, h + 1)
                total = mix_s[h, HEAD : HEAD + 1, :]
                o_ref[h, here, :] = (mix_s[h, :HEAD, :] * (1 / total)).T.astype(BF)
                lse_ref[one, here] = top_s[one, :] * SCALE + jnp.log(total)

        lax.fori_loop(0, TOKENS // B, tile, None)
        weights.next(gate, 3)
        weights.launch(up, 0)
        for r in range(4):
            weights.close(last, r)
        keep = ((q_ref, q_out), (k_ref, k_out), (v_ref, v_out), (o_ref, o_out), (a_s, a_out), (wqkv_s, wqkv_out), (wo_s, wo_out))
        keep = [pltpu.make_async_copy(s, o, ls.at[n]) for n, (s, o) in enumerate(keep)]
        for c in keep:
            c.start()
        sums = TpReduce(at, *reduce)
        mixer = wo_s[:].reshape(B, B)
        for k in range(4):
            rows = _block(sums.block(k))
            sums.add(k, _mm(jnp.concatenate([o_ref[h, rows, :] for h in range(HEADS)], axis=1), mixer))
        weights.next(up, 1)
        h = (x_ref[:].astype(F32) + _round(sums.total())).astype(BF)
        h_ref[:] = h
        b_s[:] = _normed(h.astype(F32)).astype(BF)
        states[2].start()
        weights.next(up, 2)
        weights.next(up, 3)
        states[2].middle()
        states[1].finish()
        states[2].finish()
        for n in (down, gate, up):
            for r in range(4):
                weights.close(n, r)
        for c in keep:
            c.wait()

    wqkv, last = (8, 3, *wq.shape), (8, *wo.shape)
    outs = [BLOCK, STATES, STATES, STATES, _shape(wqkv), _shape(last), *[_shape((8, *w.shape)) for w in (wg, wu, wd)], *[PER_HEAD] * 4,
            _shape((HEADS, TOKENS), F32), *[_shape((TOKENS, HEAD), F32)] * 2]
    scratch = [pltpu.VMEM((4, B, B), BF), pltpu.VMEM((B, B), BF), pltpu.VMEM(wqkv, BF), pltpu.VMEM(last, BF), *[pltpu.VMEM(PER_HEAD.shape, BF)] * 4,
               pltpu.VMEM((HEADS, B), F32), pltpu.VMEM((HEADS, HEAD + 8, B), F32), pltpu.VMEM((B, B), jnp.int32),
               *_sems((3, 3), (3, 3), (3,), (5, MOVES), (5, MOVES), (5,), (7,)), *_tp_scratch()]
    return _comm(kernel, "forward", 0, (x, dy, wq, wk, wv, wo, wg, wu, wd), outs, [INV] + [ANY] * 12 + [INV] * 3, scratch, [INV] * 9)


def _ffn(b, dy, g, u, d, h):
    chunks, per = FF // WIDE, WIDE // 256

    def kernel(b_ref, dy_ref, g_ref, u_ref, d_ref, h_ref, dh_ref, dh_out, dg_out, du_out, dd_out, early_out,
               g_s, u_s, d_s, dgate_s, dup_s, hidden_s, bt_s, dyt_s, wdt_s, wgut_s, db_s, ls, gs, gr, gl, ys, yr, *reduce):
        at = Place()
        loads = [pltpu.make_async_copy(s, o, ls.at[n]) for n, (s, o) in enumerate(((g_ref, g_s), (u_ref, u_s), (d_ref, d_s)))]
        for c in loads:
            c.start()
        at.meet(True, True)
        for c in loads:
            c.wait()
        sums = TpReduce(at, *reduce)

        def columns(j):
            return pl.ds(pl.multiple_of(j * WIDE, WIDE), WIDE)

        def prepare(j, _):
            c = columns(j)
            wdt_s[:, c] = d_s[pl.ds(j * per, per)].reshape(WIDE, B).T
            wgut_s[j, :WIDE] = g_s[:, :, c].reshape(B, WIDE).T
            wgut_s[j, WIDE:] = u_s[:, :, c].reshape(B, WIDE).T

        lax.fori_loop(0, chunks, prepare, None)

        def tile(k, _):
            t = sums.block(k)
            rows = _block(t)
            b, dy = b_ref[t], dy_ref[t]
            bt_s[:, rows] = b.T
            dyt_s[:, rows] = dy.T
            db_s[:] = jnp.zeros_like(db_s)

            def hidden(j, _):
                c = columns(j)
                gate = _mm(b, g_s[:, :, c].reshape(B, WIDE))
                up = _mm(b, u_s[:, :, c].reshape(B, WIDE))
                dh = _round(_mm(dy, wdt_s[:, c]))
                sig = jax.nn.sigmoid(gate)
                act = gate * sig
                dup = (dh * act).astype(BF)
                dgate = (dh * up * (sig + act * (1 - sig))).astype(BF)
                hidden_s[rows, c] = (act * up).astype(BF)
                dup_s[rows, c] = dup
                dgate_s[rows, c] = dgate
                db_s[:] += _mm(jnp.concatenate([dgate, dup], axis=1), wgut_s[j])

            lax.fori_loop(0, chunks, hidden, None)
            sums.add(k, db_s[:])

        lax.fori_loop(0, TOKENS // B, tile, None)
        back = _normed_bwd(h_ref[:].astype(F32), _round(sums.total()))
        dh_ref[:] = (dy_ref[at.tp].astype(F32) + _round(back)).astype(BF)
        states = TpGather(at, dh_ref, dh_out, gs, gr, gl)
        states.start()

        def down(j, _):
            d_s[pl.ds(2 * j, 2)] = _mm(dyt_s[:], hidden_s[:, _block(j)]).T.astype(BF).reshape(2, B // 2, B)

        lax.fori_loop(0, FF // B, down, None)
        stores = [pltpu.make_async_copy(s, o, ls.at[n]) for n, (s, o) in enumerate(((g_s, dg_out), (u_s, du_out), (d_s, dd_out)))]
        stores[2].start()

        def across(z):
            return [_send(d_s.at[at.other_row + d], early_out.at[d], ys.at[i], yr.at[i], at.to_y) for i, d in enumerate(ORDER[z][:EARLY])]

        for z in range(4):

            @pl.when(at.z == z)
            def _():
                for c in across(z):
                    c.start()

        for term, out in ((dgate_s, g_s), (dup_s, u_s)):

            def gate_up(j, _):
                out[:, :, _block(j)] = _mm(bt_s[:], term[:, _block(j)]).astype(BF).reshape(8, B // 8, B)

            lax.fori_loop(0, FF // B, gate_up, None)
            if out is g_s:
                stores[0].start()
                states.middle()
        stores[1].start()
        states.finish()
        for z in range(4):

            @pl.when(at.z == z)
            def _():
                for c in across(z):
                    c.wait()

        for c in stores:
            c.wait()

    wide, tall, big = pltpu.VMEM((B, FF), BF), pltpu.VMEM(g.shape, BF), pltpu.VMEM((TOKENS, FF), BF)
    scratch = [tall, tall, pltpu.VMEM(d.shape, BF), big, big, big, wide, wide, wide, pltpu.VMEM((chunks, 2 * WIDE, B), BF), pltpu.VMEM((B, B), F32),
               *_sems((3,), (3,), (3,), (), (EARLY,), (EARLY,)), *_tp_scratch()]
    outs = [BLOCK, STATES, _shape(g.shape), _shape(u.shape), _shape(d.shape), _shape((4, *d.shape[1:]))]
    return _comm(kernel, "ffn", 3, (b, dy, g, u, d, h), outs, [INV] + [ANY] * 5, scratch, [INV] * 2 + [ANY] * 3 + [INV])


def _back(dh, a, wqkv, wo, cos, sin, q, k, v, heads, lse, early, parts):
    e = SCALE * LOG2E
    count = len(parts)

    def kernel(dh_s, a_ref, wqkv_ref, wo_ref, cos_ref, sin_ref, q_ref, k_ref, v_ref, o_ref, lse_ref, early_ref, *refs):
        parts_ref, (da_ref, dwq_ref, dwk_ref, dwv_ref, dwo_ref, *refs) = refs[:count], refs[count:]
        outs, (do_s, dq_s, dk_s, dv_s, gap_s, acc_s, *refs) = refs[:count], refs[count:]
        scratch, (ds, dr, dl) = refs[: 4 * count], refs[4 * count :]
        at = Place()
        at.meet(True, False)
        sums = DpReduce(at, parts_ref, [scratch[4 * n : 4 * n + 4] for n in range(count)], ds, dr, dl, early_ref)
        sums.start()
        gap_s[:] = _gap((B, B))
        acc_s[:] = jnp.zeros_like(acc_s)
        dk_s[:] = jnp.zeros_like(dk_s)
        dv_s[:] = jnp.zeros_like(dv_s)
        sums.ready()

        def tile(i, _):
            t = 3 - i
            here = _block(t)

            pl.when(i == 0)(lambda: sums.stage(0, 0))
            pl.when(i == 1)(lambda: sums.stage(1, 1))

            @pl.when(i == 2)
            def _():
                sums.stage(0, 2)
                sums.stage(1, 2)

            pl.when(i == 3)(lambda: sums.stage(2, 2))
            dh = dh_s[t]
            mixed = [o_ref[h, here, :] for h in range(HEADS)]
            acc_s[3] += _tm(jnp.concatenate(mixed, axis=1), dh)
            do_s[:] = _mt(dh, wo_ref[:].reshape(B, B)).astype(BF)
            dos = _heads(do_s)
            deltas = [(x.astype(F32) * y.astype(F32)).T.sum(axis=0, keepdims=True) for x, y in zip(dos, mixed)]
            lses = [lse_ref[h : h + 1, here] * LOG2E for h in range(HEADS)]
            dq_s[:] = jnp.zeros_like(dq_s)

            def block(j, masked):
                keys = _block(j)
                scores = [_mt(k_ref[h, keys, :], q_ref[h, here, :]) for h in range(HEADS)]
                dps = [_mt(v_ref[h, keys, :], do_s[:, h * HEAD : (h + 1) * HEAD]) for h in range(HEADS)]
                for h in range(HEADS):
                    p = jnp.exp2(scores[h] * e - lses[h])
                    if masked:
                        p = jnp.where(gap_s[:] >= 0, p, 0.0)
                    ds = (p * (dps[h] - deltas[h])).astype(BF)
                    dv_s[h, keys, :] += _mm(p.astype(BF), do_s[:, h * HEAD : (h + 1) * HEAD])
                    dk_s[h, keys, :] += _mm(ds, q_ref[h, here, :])
                    dq_s[h] += _mm(k_ref[h, keys, :].T, ds)

            def whole(j, _):
                pl.when(jnp.logical_and(i == 0, j == 1))(lambda: sums.stage(1, 0))

                @pl.when(jnp.logical_and(i == 0, j == 2))
                def _():
                    sums.stage(2, 0)
                    sums.stage(0, 1)

                pl.when(jnp.logical_and(i == 1, j == 1))(lambda: sums.stage(2, 1))
                block(j, False)

            lax.fori_loop(0, t, whole, None)
            block(t, True)
            c, s = cos_ref[here, :], -sin_ref[here, :]
            da = jnp.zeros((B, B), F32)
            for n, ref in enumerate((dq_s, dk_s, dv_s)):
                g = []
                for h in range(HEADS):
                    one = dq_s[h].T if ref is dq_s else ref[h, here, :]
                    g.append(one.astype(BF) if ref is dv_s else _turn(_round(one * SCALE), c, s).astype(BF))
                g = jnp.concatenate(g, axis=1)
                da += _mt(g, wqkv_ref[:, n].reshape(B, B))
                acc_s[n] += _tm(a_ref[t], g)
            da_ref[t] = da.astype(BF)

        lax.fori_loop(0, TOKENS // B, tile, None)
        for n, ref in enumerate((dwq_ref, dwk_ref, dwv_ref, dwo_ref)):
            ref[:] = acc_s[n].astype(BF)
        sums.finish(outs)

    blocks = [p.shape[1:] for p in parts]
    scratch = [pltpu.VMEM((B, B), BF), pltpu.VMEM((HEADS, HEAD, B), F32), pltpu.VMEM(PER_HEAD.shape, F32), pltpu.VMEM(PER_HEAD.shape, F32),
               pltpu.VMEM((B, B), jnp.int32), pltpu.VMEM((4, B, B), F32), *_reduce_scratch(blocks), *_reduce_sems(count)]
    return _comm(kernel, "back", 4, (dh, a, wqkv, wo, cos, sin, q, k, v, heads, lse, early, *parts), [STATES, *[BLOCK] * 4, *map(_shape, blocks)], [INV] * (5 + count), scratch,
                 [INV] * 11 + [ANY] * (1 + count))


def _finish(da, x, dh, parts):
    count = len(parts)

    def kernel(da_ref, x_ref, dh_ref, *refs):
        parts_ref, (dx_ref, *refs) = refs[:count], refs[count:]
        outs, (*refs, ds, dr, dl) = refs[:count], refs[count:]
        tp = len(refs) - 4 * count
        reduce, scratch = refs[:tp], refs[tp:]
        at = Place()
        at.meet(True, True)
        weights = DpReduce(at, parts_ref, [scratch[4 * n : 4 * n + 4] for n in range(count)], ds, dr, dl)
        weights.start()
        sums = TpReduce(at, *reduce)
        for k in range(4):
            sums.add(k, da_ref[sums.block(k)].astype(F32))
        weights.ready()
        for s in range(2):
            for n in range(count):
                weights.stage(n, s)
        back = _normed_bwd(x_ref[:].astype(F32), _round(sums.total()))
        dx_ref[:] = (dh_ref[:].astype(F32) + _round(back)).astype(BF)
        for n in range(count):
            weights.stage(n, 2)
        weights.finish(outs)

    blocks = [p.shape[1:] for p in parts]
    scratch = [*_tp_scratch(), *_reduce_scratch(blocks), *_reduce_sems(count)]
    return _comm(kernel, "finish", 5, (da, x, dh, *parts), [BLOCK, *map(_shape, blocks)], [INV] * (1 + count), scratch, [INV] * 3 + [ANY] * count)


def _copies(arrays):
    count = len(arrays)

    def kernel(*refs):
        for a, b in zip(refs[:count], refs[count:]):
            b[:] = a[:]

    return pl.pallas_call(kernel, name="copies", out_shape=[_shape(a.shape) for a in arrays], in_specs=[INV] * count, out_specs=[INV] * count)(*arrays)


def solution(mesh):
    def step(x, dy, wq, wk, wv, wo, wg, wu, wd):
        x, dy = x[0], dy[0]
        h, b, a, all_dy, wqkv, wo, g, u, d, q, k, v, heads, lse, cos, sin = _forward(x, dy, wq, wk, wv, wo, wg, wu, wd)
        dh, all_dh, dg, du, dd, early = _ffn(b, all_dy, g, u, d, h)
        da, *more = _back(all_dh, a, wqkv, wo, cos, sin, q, k, v, heads, lse, early, (dd, dg, du))
        dx, dwq, dwk, dwv, dwo, dd, dg, du = _copies([*_finish(da, x, dh, [w.reshape(8, B // 8, B) for w in more[:4]]), *more[4:]])
        return dx[None], dwq, dwk, dwv, dwo, dg, du, dd

    states, by_columns, by_rows = P("dp", "tp", None), P("dp", "tp"), P(("tp", "dp"), None)
    weights = (by_columns, by_columns, by_columns, by_rows, by_columns, by_columns, by_rows)
    return jax.shard_map(step, mesh=mesh, in_specs=(states, states, *weights), out_specs=(states, *weights), check_vma=False)
```

```python
import functools

import jax
import jax.numpy as jnp
from jax import lax
from jax.experimental import pallas as pl
from jax.experimental.pallas import tpu as pltpu
from jax.sharding import PartitionSpec as P

HEADS, HEAD, THETA = 4, 128, 10000
HALF = HEAD // 2
B = 512
TOKENS, FF, WIDE = 2048, 2048, 256
NEG, HIDDEN = -1e30, -2e30
LOG2E = 1.4426950408889634
SCALE = HEAD**-0.5
F32, BF = jnp.float32, jnp.bfloat16
MESH = pl.DeviceIdType.MESH
ROOM = 67043328
ANY = pl.BlockSpec(memory_space=pl.ANY)
INV = pl.BlockSpec(memory_space=pltpu.VMEM)
EARLY = 3
RIGHT, LEFT, Y, YL, YR, MOVES = 0, 3, 6, 7, 10, 13


def _dot(a, b, ca, cb):
    return lax.dot_general(a, b, (((ca,), (cb,)), ((), ())), preferred_element_type=F32)


def _mm(a, b):
    return _dot(a, b, 1, 0)


def _mt(a, b):
    return _dot(a, b, 1, 1)


def _tm(a, b):
    return _dot(a, b, 0, 0)


def _normed(wide):
    return wide * lax.rsqrt(jnp.mean(wide * wide, -1, keepdims=True) + 1e-6)


def _normed_bwd(wide, g):
    r = lax.rsqrt(jnp.mean(wide * wide, -1, keepdims=True) + 1e-6)
    return g * r - wide * (r * r * r * jnp.mean(g * wide, -1, keepdims=True))


def _round(t):
    return t.astype(BF).astype(F32)


def _block(i):
    return pl.ds(pl.multiple_of(i * B, B), B)


def _send(src, dst, ss, rs, where):
    return pltpu.make_async_remote_copy(src_ref=src, dst_ref=dst, send_sem=ss, recv_sem=rs, device_id=where, device_id_type=MESH)


class Place:
    def __init__(self):
        self.dp, self.tp = lax.axis_index("dp"), lax.axis_index("tp")
        self.z, self.y = lax.rem(self.dp, 4), lax.div(self.dp, 4)
        self.row = self.y * 4
        self.other_row = 4 - self.row
        self.across = lax.rem(self.tp + 2, 4)
        self.core = self.tp + 1 - 2 * lax.rem(self.tp, 2)
        self.diagonal = 3 - self.tp
        self.to_y = {"dp": self.other_row + self.z, "tp": self.tp}
        self.to_right = {"dp": self.dp + 1, "tp": self.tp}
        self.to_left = {"dp": self.dp - 1, "tp": self.tp}
        self.to_across = {"dp": self.dp, "tp": self.across}
        self.to_core = {"dp": self.dp, "tp": self.core}

    def meet(self, dp, tp):
        bar = pltpu.get_barrier_semaphore()
        tell = lambda where: pl.semaphore_signal(bar, inc=1, device_id=where, device_id_type=MESH)
        count = 0
        if tp:
            tell(self.to_across)
            tell(self.to_core)
            count += 2
        if dp:
            tell(self.to_y)
            count += 1

            @pl.when(self.z > 0)
            def _():
                tell(self.to_left)

            @pl.when(self.z < 3)
            def _():
                tell(self.to_right)

            count += 1 + lax.div(self.z * (3 - self.z) + 1, 2)

        pl.semaphore_wait(bar, count)


class TpGather:
    def __init__(self, at, src, out, ss, rs, ls):
        self.own = None if src is None else pltpu.make_async_copy(src, out.at[at.tp], ls)
        src = out.at[at.tp] if src is None else src
        self.a = _send(src, out.at[at.tp], ss.at[0], rs.at[0], at.to_across)
        self.c = _send(src, out.at[at.tp], ss.at[1], rs.at[1], at.to_core)
        self.f = _send(out.at[at.across], out.at[at.across], ss.at[2], rs.at[2], at.to_core)

    def start(self):
        self.a.start()
        self.c.start()
        if self.own is not None:
            self.own.start()

    def middle(self):
        self.a.wait_recv()
        self.f.start()

    def finish(self):
        self.c.wait_recv()
        self.f.wait_recv()
        self.a.wait_send()
        self.c.wait_send()
        self.f.wait_send()
        if self.own is not None:
            self.own.wait()


class DpGather:
    def __init__(self, at, srcs, outs, ss, rs, ls):
        self.at, self.srcs, self.outs, self.ss, self.rs, self.ls = at, srcs, outs, ss, rs, ls

    def move(self, n, i, first, origin, where):
        to = self.outs[n].at[origin]
        src = self.srcs[n] if first and self.srcs[n] is not None else to
        return _send(src, to, self.ss.at[n, i], self.rs.at[n, i], where)

    def lines(self, n, s):
        at, first = self.at, s == 0
        yield (self.move(n, RIGHT + s, first, at.dp - s, at.to_right), jnp.logical_and(at.z >= s, at.z < 3),
               self.move(n, RIGHT + s, False, at.dp - 1 - s, at.to_right), at.z > s)
        yield (self.move(n, LEFT + s, first, at.dp + s, at.to_left), jnp.logical_and(at.z + s <= 3, at.z > 0),
               self.move(n, LEFT + s, False, at.dp + 1 + s, at.to_left), at.z + s < 3)

    def sides(self, n, r):
        at = self.at
        if r == 0:
            yield self.move(n, Y, True, at.dp, at.to_y), at.z >= 0
        else:
            yield self.move(n, YL + r - 1, False, at.dp - r, at.to_y), at.z >= r
            yield self.move(n, YR + r - 1, False, at.dp + r, at.to_y), at.z + r <= 3

    def local(self, n):
        return pltpu.make_async_copy(self.srcs[n], self.outs[n].at[self.at.dp], self.ls.at[n])

    def launch(self, n, r):
        if r < 3:
            for out, sends, _, _ in self.lines(n, r):
                pl.when(sends)(out.start)
        for out, sends in self.sides(n, r):
            pl.when(sends)(out.start)
        if r == 0 and self.srcs[n] is not None:
            self.local(n).start()

    def arrive(self, n, r):
        for _, _, got, comes in self.lines(n, r):
            pl.when(comes)(got.wait_recv)

    def close(self, n, r):
        if r < 3:
            for out, sends, _, _ in self.lines(n, r):
                pl.when(sends)(out.wait_send)
        for out, sends in self.sides(n, r):
            pl.when(sends)(out.wait)
        if r == 0 and self.srcs[n] is not None:
            self.local(n).wait()

    def next(self, n, r):
        self.arrive(n, r - 1)
        self.launch(n, r)


ORDER = ((3, 2, 1, 0), (3, 0, 2, 1), (0, 3, 1, 2), (0, 1, 2, 3))


class DpReduce:
    def __init__(self, at, parts, scratch, ss, rs, ls, early, count):
        self.at, self.parts, self.ss, self.rs, self.ls = at, parts, ss, rs, ls
        self.scratch, self.early, self.count = scratch, early, count

    def local(self, n):
        return pltpu.make_async_copy(self.parts[n].at[pl.ds(self.at.row, 4)], self.scratch[n][0], self.ls.at[n])

    def across(self, n, d):
        return _send(self.parts[n].at[self.at.other_row + d], self.scratch[n][1].at[d], self.ss.at[n, d], self.rs.at[n, d], self.at.to_y)

    def go_right(self, n, s, d):
        i = 4 + s
        return _send(self.scratch[n][0].at[d], self.scratch[n][2].at[s], self.ss.at[n, i], self.rs.at[n, i], self.at.to_right)

    def go_left(self, n, s, d):
        i = 7 + s
        return _send(self.scratch[n][0].at[d], self.scratch[n][3].at[s], self.ss.at[n, i], self.rs.at[n, i], self.at.to_left)

    def came(self, n, i):
        return n == 0 and i < self.count

    def each(self, body):
        for z in range(4):
            pl.when(self.at.z == z)(functools.partial(body, z))

    def start(self):
        for n in range(len(self.parts)):
            self.local(n).start()

        def go(z):
            for i, d in enumerate(ORDER[z]):
                for n in range(len(self.parts)):
                    if self.came(n, i):
                        pltpu.make_async_copy(self.early.at[d], self.scratch[n][1].at[d], self.rs.at[n, d]).start()
                    else:
                        self.across(n, d).start()

        self.each(go)

    def ready(self):
        for n in range(len(self.parts)):
            self.local(n).wait()

    def total(self, n, z, d, s, left, right, out):
        mine, got_y, from_left, from_right = self.scratch[n]
        if self.came(n, ORDER[z].index(d)):
            pltpu.make_async_copy(self.early.at[d], got_y.at[d], self.rs.at[n, d]).wait()
        else:
            self.across(n, d).wait_recv()
        terms = [mine.at[d], got_y.at[d]]
        if left:
            self.go_right(n, s, z).wait_recv()
            terms.append(from_left.at[s])
        if right:
            self.go_left(n, s, z).wait_recv()
            terms.append(from_right.at[s])
        size = mine.shape[1] // 4

        def rows(i, _):
            here = pl.ds(pl.multiple_of(i * size, size), size)
            out[here, :] = sum(t[here, :].astype(F32) for t in terms).astype(BF)

        lax.fori_loop(0, 4, rows, None)

    def stage(self, n, s):
        def go(z):
            mine = self.scratch[n][0]
            if z <= s and z < 3:
                d = 3 - s + z
                self.total(n, z, d, s - 1, z > 0, False, mine.at[d])
                self.go_right(n, s, d).start()
            if z + s >= 3 and z > 0:
                d = s - 3 + z
                self.total(n, z, d, s - 1, False, z < 3, mine.at[d])
                self.go_left(n, s, d).start()

        self.each(go)

    def finish(self, outs):
        def go(z):
            for n, out in enumerate(outs):
                self.total(n, z, z, 2, z > 0, z < 3, out)
                for i, d in enumerate(ORDER[z]):
                    if not self.came(n, i):
                        self.across(n, d).wait_send()
                for s in range(3):
                    if z <= s and z < 3:
                        self.go_right(n, s, z).wait_send()
                    if z + s >= 3 and z > 0:
                        self.go_left(n, s, z).wait_send()

        self.each(go)


def _reduce_scratch(shapes):
    return [pltpu.VMEM((k, *s), BF) for s in shapes for k in (4, 4, 3, 3)]


def _reduce_sems(count):
    return _sems((count, 10), (count, 10), (count,))


class TpReduce:
    def __init__(self, at, to_c, from_c, to_a, from_a, near, ss, rs):
        self.at, self.to_c, self.from_c, self.to_a, self.from_a, self.near = at, to_c, from_c, to_a, from_a, near
        self.c = [_send(to_c.at[i], from_c.at[i], ss.at[i], rs.at[i], at.to_core) for i in range(2)]
        self.a = _send(to_a, from_a, ss.at[2], rs.at[2], at.to_across)

    def block(self, k):
        x, core = lax.div(self.at.tp, 2), lax.rem(self.at.tp, 2)
        other_x, other_core = 1 - lax.div(k, 2), 1 - lax.rem(k, 2)
        return 2 * (x + (1 - 2 * x) * other_x) + core + (1 - 2 * core) * other_core

    def add(self, k, term):
        for i in range(2):

            @pl.when(k == 2 * i)
            def _():
                self.to_c[i] = term.astype(BF)
                self.c[i].start()

        @pl.when(k == 1)
        def _():
            self.c[0].wait_recv()
            self.to_a[:] = (term + self.from_c[0].astype(F32)).astype(BF)
            self.a.start()

        @pl.when(k == 3)
        def _():
            self.c[1].wait_recv()
            self.near[:] = term + self.from_c[1].astype(F32)

    def total(self):
        self.a.wait()
        for c in self.c:
            c.wait_send()
        return self.near[:] + self.from_a[:].astype(F32)


def _tp_scratch():
    one, two = (B, B), (2, B, B)
    return [pltpu.VMEM(two, BF), pltpu.VMEM(two, BF), pltpu.VMEM(one, BF), pltpu.VMEM(one, BF), pltpu.VMEM(one, F32), *_sems((3,), (3,))]


def _sems(*shapes):
    return [pltpu.SemaphoreType.DMA(s) for s in shapes]


def _shape(shape, dtype=BF):
    return jax.ShapeDtypeStruct(shape, dtype)


BLOCK, STATES = _shape((B, B)), _shape((4, B, B))
PER_HEAD = _shape((HEADS, TOKENS, HEAD))


def _comm(kernel, name, number, ins, outs, out_specs, scratch, in_specs, aliases={}):
    return pl.pallas_call(
        kernel, name=name, out_shape=outs, in_specs=in_specs, out_specs=out_specs, scratch_shapes=scratch, input_output_aliases=aliases,
        compiler_params=pltpu.CompilerParams(collective_id=number, has_side_effects=True, vmem_limit_bytes=ROOM),
    )(*ins)


def _turn(t, cos, sin):
    return t * cos + pltpu.roll(t, HALF, 1) * sin


def _gap(shape):
    return lax.broadcasted_iota(jnp.int32, shape, 1) - lax.broadcasted_iota(jnp.int32, shape, 0)


def _heads(t):
    return [t[:, h * HEAD : (h + 1) * HEAD] for h in range(HEADS)]


def _forward(x, dy, wq, wk, wv, wo, wg, wu, wd):
    e = SCALE * LOG2E

    def kernel(x_ref, dy_ref, wq_ref, wk_ref, wv_ref, wo_ref, wg_ref, wu_ref, wd_ref,
               h_ref, b_out, a_out, dy_out, wqkv_out, wo_out, g_out, u_out, d_out, q_out, k_out, v_out, o_out, lse_ref, cos_ref, sin_ref,
               a_s, b_s, wqkv_s, wo_s, q_ref, k_ref, v_ref, o_ref, top_s, mix_s, gap_s, ts, tr, tl, ds, dr, dl, ls, *reduce):
        at = Place()
        for i, w in enumerate((wq_ref, wk_ref, wv_ref)):
            wqkv_s[at.dp, i] = w[:]
        wo_s[at.dp] = wo_ref[:]
        a_s[at.tp] = _normed(x_ref[:].astype(F32)).astype(BF)
        at.meet(True, True)
        weights = DpGather(at, [None, None, wd_ref, wg_ref, wu_ref], [wqkv_s, wo_s, d_out, g_out, u_out], ds, dr, dl)
        qkv, last, down, gate, up = range(5)
        states = [TpGather(at, s, o, ts.at[n], tr.at[n], tl.at[n]) for n, (s, o) in enumerate(((None, a_s), (dy_ref, dy_out), (b_s, b_out)))]
        weights.launch(qkv, 0)
        weights.launch(last, 0)
        states[0].start()
        states[1].start()

        def table(i, _):
            rows = 256
            here = pl.ds(pl.multiple_of(i * rows, rows), rows)
            lane = lax.broadcasted_iota(jnp.int32, (rows, HEAD), 1)
            token = (lax.broadcasted_iota(jnp.int32, (rows, HEAD), 0) + i * rows).astype(F32)
            low = lane < HALF
            angle = token * jnp.exp((jnp.where(low, lane, lane - HALF).astype(F32)) * (-jnp.log(jnp.float32(THETA)) / HALF))
            cos_ref[here, :] = jnp.cos(angle)
            sine = jnp.sin(angle)
            sin_ref[here, :] = jnp.where(low, -sine, sine)

        lax.fori_loop(0, TOKENS // 256, table, None)
        gap_s[:] = _gap((B, B))
        for r in (1, 2):
            weights.next(qkv, r)
            weights.next(last, r)
        states[0].middle()
        weights.next(qkv, 3)
        weights.next(last, 3)
        weights.launch(down, 0)
        weights.launch(gate, 0)
        states[0].finish()
        for r in range(4):
            weights.close(qkv, r)

        def tile(t, _):
            here = _block(t)
            c, s = cos_ref[here, :], sin_ref[here, :]
            for i, ref in enumerate((q_ref, k_ref, v_ref)):
                all_heads = _mm(a_s[t], wqkv_s[:, i].reshape(B, B)).astype(BF)
                for h, one in enumerate(_heads(all_heads)):
                    ref[h, here, :] = one if ref is v_ref else _turn(one.astype(F32), c, s).astype(BF)
            top_s[:] = jnp.full_like(top_s, NEG)
            mix_s[:] = jnp.zeros_like(mix_s)
            ones = jnp.ones((8, B), BF)
            pl.when(t == 1)(lambda: states[1].middle())
            pl.when(t == 2)(lambda: weights.next(down, 1))
            pl.when(t == 3)(lambda: weights.next(down, 2))

            def block(j, masked):
                keys = _block(j)
                scores = [_mt(k_ref[h, keys, :], q_ref[h, here, :]) for h in range(HEADS)]
                weigh, keep = [], []
                for h, sc in enumerate(scores):
                    if masked:
                        sc = jnp.where(gap_s[:] >= 0, sc, HIDDEN)
                    one = slice(h, h + 1)
                    old = top_s[one, :]
                    top = jnp.maximum(old, sc.max(axis=0, keepdims=True))
                    top_s[one, :] = top
                    weigh.append(jnp.exp2((sc - top) * e).astype(BF))
                    keep.append(jnp.exp2((old - top) * e))
                for h in range(HEADS):
                    values = jnp.concatenate([v_ref[h, keys, :].T, ones], axis=0)
                    mix_s[h] = mix_s[h] * keep[h] + _mm(values, weigh[h])

            def whole(j, _):
                pl.when(jnp.logical_and(t == 2, j == 1))(lambda: weights.next(gate, 1))
                pl.when(jnp.logical_and(t == 3, j == 1))(lambda: weights.next(gate, 2))
                block(j, False)

            lax.fori_loop(0, t, whole, None)
            pl.when(t == 3)(lambda: weights.next(down, 3))
            block(t, True)
            for h in range(HEADS):
                one = slice(h, h + 1)
                total = mix_s[h, HEAD : HEAD + 1, :]
                o_ref[h, here, :] = (mix_s[h, :HEAD, :] * (1 / total)).T.astype(BF)
                lse_ref[one, here] = top_s[one, :] * SCALE + jnp.log(total)

        lax.fori_loop(0, TOKENS // B, tile, None)
        weights.next(gate, 3)
        weights.launch(up, 0)
        for r in range(4):
            weights.close(last, r)
        keep = ((q_ref, q_out), (k_ref, k_out), (v_ref, v_out), (o_ref, o_out), (a_s, a_out), (wqkv_s, wqkv_out), (wo_s, wo_out))
        keep = [pltpu.make_async_copy(s, o, ls.at[n]) for n, (s, o) in enumerate(keep)]
        for c in keep:
            c.start()
        sums = TpReduce(at, *reduce)
        mixer = wo_s[:].reshape(B, B)
        for k in range(4):
            rows = _block(sums.block(k))
            sums.add(k, _mm(jnp.concatenate([o_ref[h, rows, :] for h in range(HEADS)], axis=1), mixer))
        weights.next(up, 1)
        h = (x_ref[:].astype(F32) + _round(sums.total())).astype(BF)
        h_ref[:] = h
        b_s[:] = _normed(h.astype(F32)).astype(BF)
        states[2].start()
        weights.next(up, 2)
        weights.next(up, 3)
        states[2].middle()
        states[1].finish()
        states[2].finish()
        for n in (down, gate, up):
            for r in range(4):
                weights.close(n, r)
        for c in keep:
            c.wait()

    wqkv, last = (8, 3, *wq.shape), (8, *wo.shape)
    outs = [BLOCK, STATES, STATES, STATES, _shape(wqkv), _shape(last), *[_shape((8, *w.shape)) for w in (wg, wu, wd)], *[PER_HEAD] * 4,
            _shape((HEADS, TOKENS), F32), *[_shape((TOKENS, HEAD), F32)] * 2]
    scratch = [pltpu.VMEM((4, B, B), BF), pltpu.VMEM((B, B), BF), pltpu.VMEM(wqkv, BF), pltpu.VMEM(last, BF), *[pltpu.VMEM(PER_HEAD.shape, BF)] * 4,
               pltpu.VMEM((HEADS, B), F32), pltpu.VMEM((HEADS, HEAD + 8, B), F32), pltpu.VMEM((B, B), jnp.int32),
               *_sems((3, 3), (3, 3), (3,), (5, MOVES), (5, MOVES), (5,), (7,)), *_tp_scratch()]
    return _comm(kernel, "forward", 0, (x, dy, wq, wk, wv, wo, wg, wu, wd), outs, [INV] + [ANY] * 12 + [INV] * 3, scratch, [INV] * 9)


def _ffn(b, dy, g, u, d, h):
    chunks, per = FF // WIDE, WIDE // 256

    def kernel(b_ref, dy_ref, g_ref, u_ref, d_ref, h_ref, dh_ref, dh_out, dg_out, du_out, dd_out, early_out,
               g_s, u_s, d_s, dgate_s, dup_s, hidden_s, bt_s, dyt_s, wdt_s, wgut_s, db_s, ls, gs, gr, gl, ys, yr, *reduce):
        at = Place()
        loads = [pltpu.make_async_copy(s, o, ls.at[n]) for n, (s, o) in enumerate(((g_ref, g_s), (u_ref, u_s), (d_ref, d_s)))]
        for c in loads:
            c.start()
        at.meet(True, True)
        for c in loads:
            c.wait()
        sums = TpReduce(at, *reduce)

        def columns(j):
            return pl.ds(j * WIDE, WIDE) if isinstance(j, int) else pl.ds(pl.multiple_of(j * WIDE, WIDE), WIDE)

        def prepare(j, _):
            c = columns(j)
            wdt_s[:, c] = d_s[pl.ds(j * per, per)].reshape(WIDE, B).T
            wgut_s[j, :WIDE] = g_s[:, :, c].reshape(B, WIDE).T
            wgut_s[j, WIDE:] = u_s[:, :, c].reshape(B, WIDE).T

        lax.fori_loop(0, chunks, prepare, None)

        def tile(k, _):
            t = sums.block(k)
            rows = _block(t)
            b, dy = b_ref[t], dy_ref[t]
            bt_s[:, rows] = b.T
            dyt_s[:, rows] = dy.T
            db_s[:] = jnp.zeros_like(db_s)

            def hidden(j):
                c = columns(j)
                gate = _mm(b, g_s[:, :, c].reshape(B, WIDE))
                up = _mm(b, u_s[:, :, c].reshape(B, WIDE))
                dh = _round(_mm(dy, wdt_s[:, c]))
                sig = jax.nn.sigmoid(gate)
                act = gate * sig
                dup = (dh * act).astype(BF)
                dgate = (dh * up * (sig + act * (1 - sig))).astype(BF)
                hidden_s[rows, c] = (act * up).astype(BF)
                dup_s[rows, c] = dup
                dgate_s[rows, c] = dgate

            def states(j):
                c = columns(j)
                db_s[:] += _mm(jnp.concatenate([dgate_s[rows, c], dup_s[rows, c]], axis=1), wgut_s[j])

            hidden(0)
            for j in range(1, chunks):
                hidden(j)
                states(j - 1)
            states(chunks - 1)
            sums.add(k, db_s[:])

        lax.fori_loop(0, TOKENS // B, tile, None)
        back = _normed_bwd(h_ref[:].astype(F32), _round(sums.total()))
        dh_ref[:] = (dy_ref[at.tp].astype(F32) + _round(back)).astype(BF)
        states = TpGather(at, dh_ref, dh_out, gs, gr, gl)
        states.start()

        def down(i, _):
            j = lax.rem(i + lax.div(at.other_row, 2), 4)
            d_s[pl.ds(2 * j, 2)] = _mm(dyt_s[:], hidden_s[:, _block(j)]).T.astype(BF).reshape(2, B // 2, B)

        lax.fori_loop(0, 2, down, None)
        stores = [pltpu.make_async_copy(s, o, ls.at[n]) for n, (s, o) in enumerate(((g_s, dg_out), (u_s, du_out), (d_s, dd_out)))]

        def across(z):
            return [_send(d_s.at[at.other_row + d], early_out.at[d], ys.at[i], yr.at[i], at.to_y) for i, d in enumerate(ORDER[z][:EARLY])]

        for z in range(4):

            @pl.when(at.z == z)
            def _():
                for c in across(z):
                    c.start()

        lax.fori_loop(2, 4, down, None)
        stores[2].start()
        for term, out in ((dgate_s, g_s), (dup_s, u_s)):

            def gate_up(j, _):
                out[:, :, _block(j)] = _mm(bt_s[:], term[:, _block(j)]).astype(BF).reshape(8, B // 8, B)

            lax.fori_loop(0, FF // B, gate_up, None)
            if out is g_s:
                stores[0].start()
                states.middle()
        stores[1].start()
        states.finish()
        for z in range(4):

            @pl.when(at.z == z)
            def _():
                for c in across(z):
                    c.wait()

        for c in stores:
            c.wait()

    wide, tall, big = pltpu.VMEM((B, FF), BF), pltpu.VMEM(g.shape, BF), pltpu.VMEM((TOKENS, FF), BF)
    scratch = [tall, tall, pltpu.VMEM(d.shape, BF), big, big, big, wide, wide, wide, pltpu.VMEM((chunks, 2 * WIDE, B), BF), pltpu.VMEM((B, B), F32),
               *_sems((3,), (3,), (3,), (), (EARLY,), (EARLY,)), *_tp_scratch()]
    outs = [BLOCK, STATES, _shape(g.shape), _shape(u.shape), _shape(d.shape), _shape((4, *d.shape[1:]))]
    return _comm(kernel, "ffn", 3, (b, dy, g, u, d, h), outs, [INV] + [ANY] * 5, scratch, [INV] * 2 + [ANY] * 3 + [INV])


def _back(dh, a, wqkv, wo, cos, sin, q, k, v, heads, lse, early, parts):
    e = SCALE * LOG2E
    count = len(parts)

    def kernel(*refs):
        given, (early_ref, *refs) = refs[: len(held)], refs[len(held) :]
        parts_ref, (da_ref, dwq_ref, dwk_ref, dwv_ref, dwo_out, early_out, *refs) = refs[:count], refs[count:]
        outs, (hs, dwo_s, ws, wr, wl, *refs) = refs[:count], refs[count:]
        here, (do_s, dq_s, dk_s, dv_s, gap_s, acc_s, *refs) = refs[: len(held)], refs[len(held) :]
        dh_s, a_ref, wqkv_ref, wo_ref, cos_ref, sin_ref, q_ref, k_ref, v_ref, o_ref, lse_ref = here
        loads = [pltpu.make_async_copy(s, o, hs.at[n]) for n, (s, o) in enumerate(zip(given, here))]
        scratch, (ds, dr, dl) = refs[: 4 * count], refs[4 * count :]
        at = Place()
        at.meet(True, False)
        sums = DpReduce(at, parts_ref, [scratch[4 * n : 4 * n + 4] for n in range(count)], ds, dr, dl, early_ref, EARLY)
        sums.start()
        for c in loads:
            c.start()
        gap_s[:] = _gap((B, B))
        acc_s[:] = jnp.zeros_like(acc_s)
        dk_s[:] = jnp.zeros_like(dk_s)
        dv_s[:] = jnp.zeros_like(dv_s)
        sums.ready()
        sums.stage(0, 0)
        for c in loads:
            c.wait()
        mixed = [jnp.concatenate([o_ref[h, _block(t), :] for h in range(HEADS)], axis=1) for t in range(4)]
        dwo_s[:] = sum(_tm(m, dh_s[t]) for t, m in enumerate(mixed)).astype(BF).reshape(dwo_s.shape)
        mix_store = pltpu.make_async_copy(dwo_s, dwo_out, wl)
        mix_store.start()
        mix_sends = [_send(dwo_s.at[at.other_row + d], early_out.at[d], ws.at[d], wr.at[d], at.to_y) for d in range(4)]
        for c in mix_sends:
            c.start()

        def tile(i, _):
            t = 3 - i
            here = _block(t)


            @pl.when(i == 1)
            def _():
                sums.stage(0, 2)
                sums.stage(1, 1)

            pl.when(i == 2)(lambda: sums.stage(1, 2))
            pl.when(i == 3)(lambda: sums.stage(2, 2))
            dh = dh_s[t]
            mixed = [o_ref[h, here, :] for h in range(HEADS)]
            do_s[:] = _mt(dh, wo_ref[:].reshape(B, B)).astype(BF)
            dos = _heads(do_s)
            deltas = [(x.astype(F32) * y.astype(F32)).T.sum(axis=0, keepdims=True) for x, y in zip(dos, mixed)]
            lses = [lse_ref[h : h + 1, here] * LOG2E for h in range(HEADS)]
            dq_s[:] = jnp.zeros_like(dq_s)

            def block(j, masked):
                keys = _block(j)
                scores = [_mt(k_ref[h, keys, :], q_ref[h, here, :]) for h in range(HEADS)]
                dps = [_mt(v_ref[h, keys, :], do_s[:, h * HEAD : (h + 1) * HEAD]) for h in range(HEADS)]
                for h in range(HEADS):
                    p = jnp.exp2(scores[h] * e - lses[h])
                    if masked:
                        p = jnp.where(gap_s[:] >= 0, p, 0.0)
                    ds = (p * (dps[h] - deltas[h])).astype(BF)
                    dv_s[h, keys, :] += _mm(p.astype(BF), do_s[:, h * HEAD : (h + 1) * HEAD])
                    dk_s[h, keys, :] += _mm(ds, q_ref[h, here, :])
                    dq_s[h] += _mm(k_ref[h, keys, :].T, ds)

            def whole(j, _):
                @pl.when(jnp.logical_and(i == 0, j == 1))
                def _():
                    sums.stage(0, 1)
                    sums.stage(1, 0)

                pl.when(jnp.logical_and(i == 0, j == 2))(lambda: sums.stage(2, 0))
                pl.when(jnp.logical_and(i == 1, j == 1))(lambda: sums.stage(2, 1))
                block(j, False)

            lax.fori_loop(0, t, whole, None)
            block(t, True)
            c, s = cos_ref[here, :], -sin_ref[here, :]
            da = jnp.zeros((B, B), F32)
            for n, ref in enumerate((dq_s, dk_s, dv_s)):
                g = []
                for h in range(HEADS):
                    one = dq_s[h].T if ref is dq_s else ref[h, here, :]
                    g.append(one.astype(BF) if ref is dv_s else _turn(_round(one * SCALE), c, s).astype(BF))
                g = jnp.concatenate(g, axis=1)
                da += _mt(g, wqkv_ref[:, n].reshape(B, B))
                acc_s[n] += _tm(a_ref[t], g)
            da_ref[t] = da.astype(BF)

        lax.fori_loop(0, TOKENS // B, tile, None)
        for n, ref in enumerate((dwq_ref, dwk_ref, dwv_ref)):
            ref[:] = acc_s[n].astype(BF)
        sums.finish(outs)
        mix_store.wait()
        for c in mix_sends:
            c.wait()

    held = (dh, a, wqkv, wo, cos, sin, q, k, v, heads, lse)
    blocks = [p.shape[1:] for p in parts]
    scratch = [*_sems((len(held),)), pltpu.VMEM(wo.shape, BF), *_sems((4,), (4,), ()), *[pltpu.VMEM(t.shape, t.dtype) for t in held], pltpu.VMEM((B, B), BF), pltpu.VMEM((HEADS, HEAD, B), F32), pltpu.VMEM(PER_HEAD.shape, F32), pltpu.VMEM(PER_HEAD.shape, F32),
               pltpu.VMEM((B, B), jnp.int32), pltpu.VMEM((3, B, B), F32), *_reduce_scratch(blocks), *_reduce_sems(count)]
    return _comm(kernel, "back", 4, (*held, early, *parts), [STATES, *[BLOCK] * 3, _shape(wo.shape), _shape((4, *wo.shape[1:])), *map(_shape, blocks)], [INV] * 4 + [ANY] * 2 + [INV] * count, scratch,
                 [ANY] * (len(held) + 1 + count))


def _finish(da, x, dh, early, parts):
    count = len(parts)

    def kernel(da_ref, x_ref, dh_ref, early_ref, *refs):
        parts_ref, (dx_ref, *refs) = refs[:count], refs[count:]
        outs, (*refs, ds, dr, dl) = refs[:count], refs[count:]
        tp = len(refs) - 4 * count
        reduce, scratch = refs[:tp], refs[tp:]
        at = Place()
        at.meet(True, True)
        weights = DpReduce(at, parts_ref, [scratch[4 * n : 4 * n + 4] for n in range(count)], ds, dr, dl, early_ref, 4)
        weights.start()
        weights.ready()
        weights.stage(0, 0)
        sums = TpReduce(at, *reduce)
        for k in range(4):
            sums.add(k, da_ref[sums.block(k)].astype(F32))
        for s in range(3):
            for n in range(count):
                if s + n > 0:
                    weights.stage(n, s)
        back = _normed_bwd(x_ref[:].astype(F32), _round(sums.total()))
        dx_ref[:] = (dh_ref[:].astype(F32) + _round(back)).astype(BF)
        weights.finish(outs)

    blocks = [p.shape[1:] for p in parts]
    scratch = [*_tp_scratch(), *_reduce_scratch(blocks), *_reduce_sems(count)]
    return _comm(kernel, "finish", 5, (da, x, dh, early, *parts), [BLOCK, *map(_shape, blocks)], [INV] * (1 + count), scratch, [INV] * 3 + [ANY] * (1 + count))


def _copies(arrays):
    count = len(arrays)

    def kernel(*refs):
        for a, b in zip(refs[:count], refs[count:]):
            b[:] = a[:]

    return pl.pallas_call(kernel, name="copies", out_shape=[_shape(a.shape) for a in arrays], in_specs=[INV] * count, out_specs=[INV] * count)(*arrays)


def solution(mesh):
    def step(x, dy, wq, wk, wv, wo, wg, wu, wd):
        x, dy = x[0], dy[0]
        h, b, a, all_dy, wqkv, wo, g, u, d, q, k, v, heads, lse, cos, sin = _forward(x, dy, wq, wk, wv, wo, wg, wu, wd)
        dh, all_dh, dg, du, dd, early = _ffn(b, all_dy, g, u, d, h)
        da, dwq, dwk, dwv, dwo, early, *more = _back(all_dh, a, wqkv, wo, cos, sin, q, k, v, heads, lse, early, (dd, dg, du))
        parts = [dwo, *[w.reshape(wo.shape) for w in (dwq, dwk, dwv)]]
        dx, dwo, dwq, dwk, dwv, dd, dg, du = _copies([*_finish(da, x, dh, early, parts), *more])
        return dx[None], dwq, dwk, dwv, dwo, dg, du, dd

    states, by_columns, by_rows = P("dp", "tp", None), P("dp", "tp"), P(("tp", "dp"), None)
    weights = (by_columns, by_columns, by_columns, by_rows, by_columns, by_columns, by_rows)
    return jax.shard_map(step, mesh=mesh, in_specs=(states, states, *weights), out_specs=(states, *weights), check_vma=False)
```

```python
import functools

import jax
import jax.numpy as jnp
from jax import lax
from jax.experimental import pallas as pl
from jax.experimental.pallas import tpu as pltpu
from jax.sharding import PartitionSpec as P

HEADS, HEAD, THETA = 4, 128, 10000
HALF = HEAD // 2
B = 512
TOKENS, FF, WIDE = 2048, 2048, 256
NEG, HIDDEN = -1e30, -2e30
LOG2E = 1.4426950408889634
SCALE = HEAD**-0.5
F32, BF = jnp.float32, jnp.bfloat16
MESH = pl.DeviceIdType.MESH
ROOM = 67043328
ANY = pl.BlockSpec(memory_space=pl.ANY)
INV = pl.BlockSpec(memory_space=pltpu.VMEM)
EARLY = 3
RIGHT, LEFT, Y, YL, YR, MOVES = 0, 3, 6, 7, 10, 13


def _dot(a, b, ca, cb):
    return lax.dot_general(a, b, (((ca,), (cb,)), ((), ())), preferred_element_type=F32)


def _mm(a, b):
    return _dot(a, b, 1, 0)


def _mt(a, b):
    return _dot(a, b, 1, 1)


def _tm(a, b):
    return _dot(a, b, 0, 0)


def _normed(wide):
    return wide * lax.rsqrt(jnp.mean(wide * wide, -1, keepdims=True) + 1e-6)


def _normed_bwd(wide, g):
    r = lax.rsqrt(jnp.mean(wide * wide, -1, keepdims=True) + 1e-6)
    return g * r - wide * (r * r * r * jnp.mean(g * wide, -1, keepdims=True))


def _round(t):
    return t.astype(BF).astype(F32)


def _block(i):
    return pl.ds(pl.multiple_of(i * B, B), B)


def _send(src, dst, ss, rs, where):
    return pltpu.make_async_remote_copy(src_ref=src, dst_ref=dst, send_sem=ss, recv_sem=rs, device_id=where, device_id_type=MESH)


class Place:
    def __init__(self):
        self.dp, self.tp = lax.axis_index("dp"), lax.axis_index("tp")
        self.z, self.y = lax.rem(self.dp, 4), lax.div(self.dp, 4)
        self.row = self.y * 4
        self.other_row = 4 - self.row
        self.across = lax.rem(self.tp + 2, 4)
        self.core = self.tp + 1 - 2 * lax.rem(self.tp, 2)
        self.diagonal = 3 - self.tp
        self.to_y = {"dp": self.other_row + self.z, "tp": self.tp}
        self.to_right = {"dp": self.dp + 1, "tp": self.tp}
        self.to_left = {"dp": self.dp - 1, "tp": self.tp}
        self.to_across = {"dp": self.dp, "tp": self.across}
        self.to_core = {"dp": self.dp, "tp": self.core}

    def meet(self, dp, tp):
        bar = pltpu.get_barrier_semaphore()
        tell = lambda where: pl.semaphore_signal(bar, inc=1, device_id=where, device_id_type=MESH)
        count = 0
        if tp:
            tell(self.to_across)
            tell(self.to_core)
            count += 2
        if dp:
            tell(self.to_y)
            count += 1

            @pl.when(self.z > 0)
            def _():
                tell(self.to_left)

            @pl.when(self.z < 3)
            def _():
                tell(self.to_right)

            count += 1 + lax.div(self.z * (3 - self.z) + 1, 2)

        pl.semaphore_wait(bar, count)


class TpGather:
    def __init__(self, at, src, out, ss, rs, ls):
        self.own = None if src is None else pltpu.make_async_copy(src, out.at[at.tp], ls)
        src = out.at[at.tp] if src is None else src
        self.a = _send(src, out.at[at.tp], ss.at[0], rs.at[0], at.to_across)
        self.c = _send(src, out.at[at.tp], ss.at[1], rs.at[1], at.to_core)
        self.f = _send(out.at[at.across], out.at[at.across], ss.at[2], rs.at[2], at.to_core)

    def start(self):
        self.a.start()
        self.c.start()
        if self.own is not None:
            self.own.start()

    def middle(self):
        self.a.wait_recv()
        self.f.start()

    def finish(self):
        self.c.wait_recv()
        self.f.wait_recv()
        self.a.wait_send()
        self.c.wait_send()
        self.f.wait_send()
        if self.own is not None:
            self.own.wait()


class DpGather:
    def __init__(self, at, srcs, outs, ss, rs, ls):
        self.at, self.srcs, self.outs, self.ss, self.rs, self.ls = at, srcs, outs, ss, rs, ls

    def move(self, n, i, first, origin, where):
        to = self.outs[n](origin)
        src = self.srcs[n] if first and self.srcs[n] is not None else to
        return _send(src, to, self.ss.at[n, i], self.rs.at[n, i], where)

    def lines(self, n, s):
        at, first = self.at, s == 0
        yield (self.move(n, RIGHT + s, first, at.dp - s, at.to_right), jnp.logical_and(at.z >= s, at.z < 3),
               self.move(n, RIGHT + s, False, at.dp - 1 - s, at.to_right), at.z > s)
        yield (self.move(n, LEFT + s, first, at.dp + s, at.to_left), jnp.logical_and(at.z + s <= 3, at.z > 0),
               self.move(n, LEFT + s, False, at.dp + 1 + s, at.to_left), at.z + s < 3)

    def sides(self, n, r):
        at = self.at
        if r == 0:
            yield self.move(n, Y, True, at.dp, at.to_y), at.z >= 0
        else:
            yield self.move(n, YL + r - 1, False, at.dp - r, at.to_y), at.z >= r
            yield self.move(n, YR + r - 1, False, at.dp + r, at.to_y), at.z + r <= 3

    def local(self, n):
        return pltpu.make_async_copy(self.srcs[n], self.outs[n](self.at.dp), self.ls.at[n])

    def launch(self, n, r):
        if r < 3:
            for out, sends, _, _ in self.lines(n, r):
                pl.when(sends)(out.start)
        for out, sends in self.sides(n, r):
            pl.when(sends)(out.start)
        if r == 0 and self.srcs[n] is not None:
            self.local(n).start()

    def arrive(self, n, r):
        for _, _, got, comes in self.lines(n, r):
            pl.when(comes)(got.wait_recv)

    def close(self, n, r):
        if r < 3:
            for out, sends, _, _ in self.lines(n, r):
                pl.when(sends)(out.wait_send)
        for out, sends in self.sides(n, r):
            pl.when(sends)(out.wait)
        if r == 0 and self.srcs[n] is not None:
            self.local(n).wait()

    def next(self, n, r):
        self.arrive(n, r - 1)
        self.launch(n, r)


class DpSides:
    def __init__(self, at, src, out, ss, rs, ls):
        self.at, self.src, self.out, self.ss, self.rs = at, src, out, ss, rs
        self.y = _send(src, out(at.dp), ss.at[Y], rs.at[Y], at.to_y)
        self.own = pltpu.make_async_copy(src, out(at.dp), ls)

    def start(self):
        self.y.start()
        self.own.start()

    def lines(self, row, s):
        at = self.at
        first = row == 0
        base = at.dp if first else at.other_row + at.z
        numbers = (RIGHT, LEFT) if first else (YL, YR)
        for i, step, sends, comes in ((numbers[0], -1, jnp.logical_and(at.z >= s, at.z < 3), at.z > s),
                                      (numbers[1], 1, jnp.logical_and(at.z + s <= 3, at.z > 0), at.z + s < 3)):
            to = at.to_right if step < 0 else at.to_left
            out, came = self.out(base + step * s), self.out(base + step * (s + 1))
            src = self.src if first and s == 0 else out
            yield (_send(src, out, self.ss.at[i + s], self.rs.at[i + s], to), sends, _send(came, came, self.ss.at[i + s], self.rs.at[i + s], to), comes)

    def launch(self, row, s):
        if s == 0 and row == 1:
            self.y.wait_recv()
        if s > 0:
            self.arrive(row, s - 1)
        for out, sends, _, _ in self.lines(row, s):
            pl.when(sends)(out.start)

    def arrive(self, row, s):
        for _, _, got, comes in self.lines(row, s):
            pl.when(comes)(got.wait_recv)

    def close(self):
        for row in range(2):
            self.arrive(row, 2)
            for s in range(3):
                for out, sends, _, _ in self.lines(row, s):
                    pl.when(sends)(out.wait_send)
        self.y.wait_send()
        self.own.wait()


ORDER = ((3, 2, 1, 0), (3, 0, 2, 1), (0, 3, 1, 2), (0, 1, 2, 3))


class DpReduce:
    def __init__(self, at, parts, scratch, ss, rs, ls, early, count):
        self.at, self.parts, self.ss, self.rs, self.ls = at, parts, ss, rs, ls
        self.scratch, self.early, self.count = scratch, early, count

    def local(self, n):
        return pltpu.make_async_copy(self.parts[n].at[pl.ds(self.at.row, 4)], self.scratch[n][0], self.ls.at[n])

    def across(self, n, d):
        return _send(self.parts[n].at[self.at.other_row + d], self.scratch[n][1].at[d], self.ss.at[n, d], self.rs.at[n, d], self.at.to_y)

    def go_right(self, n, s, d):
        i = 4 + s
        return _send(self.scratch[n][0].at[d], self.scratch[n][2].at[s], self.ss.at[n, i], self.rs.at[n, i], self.at.to_right)

    def go_left(self, n, s, d):
        i = 7 + s
        return _send(self.scratch[n][0].at[d], self.scratch[n][3].at[s], self.ss.at[n, i], self.rs.at[n, i], self.at.to_left)

    def came(self, n, i):
        return n == 0 and i < self.count

    def each(self, body):
        for z in range(4):
            pl.when(self.at.z == z)(functools.partial(body, z))

    def start(self):
        for n in range(len(self.parts)):
            self.local(n).start()

        def go(z):
            for i, d in enumerate(ORDER[z]):
                for n in range(len(self.parts)):
                    if self.came(n, i):
                        pltpu.make_async_copy(self.early.at[d], self.scratch[n][1].at[d], self.rs.at[n, d]).start()
                    else:
                        self.across(n, d).start()

        self.each(go)

    def ready(self):
        for n in range(len(self.parts)):
            self.local(n).wait()

    def total(self, n, z, d, s, left, right, out):
        mine, got_y, from_left, from_right = self.scratch[n]
        if self.came(n, ORDER[z].index(d)):
            pltpu.make_async_copy(self.early.at[d], got_y.at[d], self.rs.at[n, d]).wait()
        else:
            self.across(n, d).wait_recv()
        terms = [mine.at[d], got_y.at[d]]
        if left:
            self.go_right(n, s, z).wait_recv()
            terms.append(from_left.at[s])
        if right:
            self.go_left(n, s, z).wait_recv()
            terms.append(from_right.at[s])
        size = mine.shape[1] // 4

        def rows(i, _):
            here = pl.ds(pl.multiple_of(i * size, size), size)
            out[here, :] = sum(t[here, :].astype(F32) for t in terms).astype(BF)

        lax.fori_loop(0, 4, rows, None)

    def stage(self, n, s):
        def go(z):
            mine = self.scratch[n][0]
            if z <= s and z < 3:
                d = 3 - s + z
                self.total(n, z, d, s - 1, z > 0, False, mine.at[d])
                self.go_right(n, s, d).start()
            if z + s >= 3 and z > 0:
                d = s - 3 + z
                self.total(n, z, d, s - 1, False, z < 3, mine.at[d])
                self.go_left(n, s, d).start()

        self.each(go)

    def finish(self, outs):
        def go(z):
            for n, out in enumerate(outs):
                self.total(n, z, z, 2, z > 0, z < 3, out)
                for i, d in enumerate(ORDER[z]):
                    if not self.came(n, i):
                        self.across(n, d).wait_send()
                for s in range(3):
                    if z <= s and z < 3:
                        self.go_right(n, s, z).wait_send()
                    if z + s >= 3 and z > 0:
                        self.go_left(n, s, z).wait_send()

        self.each(go)


def _reduce_scratch(shapes):
    return [pltpu.VMEM((k, *s), BF) for s in shapes for k in (4, 4, 3, 3)]


def _reduce_sems(count):
    return _sems((count, 10), (count, 10), (count,))


class TpReduce:
    def __init__(self, at, to_c, from_c, to_a, from_a, near, ss, rs):
        self.at, self.to_c, self.from_c, self.to_a, self.from_a, self.near = at, to_c, from_c, to_a, from_a, near
        self.c = [_send(to_c.at[i], from_c.at[i], ss.at[i], rs.at[i], at.to_core) for i in range(2)]
        self.a = _send(to_a, from_a, ss.at[2], rs.at[2], at.to_across)

    def block(self, k):
        x, core = lax.div(self.at.tp, 2), lax.rem(self.at.tp, 2)
        other_x, other_core = 1 - lax.div(k, 2), 1 - lax.rem(k, 2)
        return 2 * (x + (1 - 2 * x) * other_x) + core + (1 - 2 * core) * other_core

    def add(self, k, term):
        for i in range(2):

            @pl.when(k == 2 * i)
            def _():
                self.to_c[i] = term.astype(BF)
                self.c[i].start()

        @pl.when(k == 1)
        def _():
            self.c[0].wait_recv()
            self.to_a[:] = (term + self.from_c[0].astype(F32)).astype(BF)
            self.a.start()

        @pl.when(k == 3)
        def _():
            self.c[1].wait_recv()
            self.near[:] = term + self.from_c[1].astype(F32)

    def total(self):
        self.a.wait()
        for c in self.c:
            c.wait_send()
        return self.near[:] + self.from_a[:].astype(F32)


def _tp_scratch():
    one, two = (B, B), (2, B, B)
    return [pltpu.VMEM(two, BF), pltpu.VMEM(two, BF), pltpu.VMEM(one, BF), pltpu.VMEM(one, BF), pltpu.VMEM(one, F32), *_sems((3,), (3,))]


def _sems(*shapes):
    return [pltpu.SemaphoreType.DMA(s) for s in shapes]


def _shape(shape, dtype=BF):
    return jax.ShapeDtypeStruct(shape, dtype)


BLOCK, STATES = _shape((B, B)), _shape((4, B, B))
PER_HEAD = _shape((HEADS, TOKENS, HEAD))


def _comm(kernel, name, number, ins, outs, out_specs, scratch, in_specs, aliases={}):
    return pl.pallas_call(
        kernel, name=name, out_shape=outs, in_specs=in_specs, out_specs=out_specs, scratch_shapes=scratch, input_output_aliases=aliases,
        compiler_params=pltpu.CompilerParams(collective_id=number, has_side_effects=True, vmem_limit_bytes=ROOM),
    )(*ins)


def _turn(t, cos, sin):
    return t * cos + pltpu.roll(t, HALF, 1) * sin


def _gap(shape):
    return lax.broadcasted_iota(jnp.int32, shape, 1) - lax.broadcasted_iota(jnp.int32, shape, 0)


def _heads(t):
    return [t[:, h * HEAD : (h + 1) * HEAD] for h in range(HEADS)]


def _forward(x, dy, wq, wk, wv, wo, wg, wu, wd):
    e = SCALE * LOG2E

    def kernel(x_ref, dy_ref, wq_ref, wk_ref, wv_ref, wo_ref, wg_ref, wu_ref, wd_ref,
               h_ref, b_out, a_out, dy_out, wqkv_out, wo_out, g_out, u_out, d_out, q_out, k_out, v_out, o_out, lse_ref, cos_ref, sin_ref,
               a_s, b_s, wqkv_s, wo_s, q_ref, k_ref, v_ref, o_ref, top_s, mix_s, gap_s, ts, tr, tl, ds, dr, dl, es, er, el, ls, *reduce):
        at = Place()
        for i, w in enumerate((wq_ref, wk_ref, wv_ref)):
            wqkv_s[at.dp, i] = w[:]
        wo_s[at.dp] = wo_ref[:]
        a_s[at.tp] = _normed(x_ref[:].astype(F32)).astype(BF)
        at.meet(True, True)
        half = wd_ref.shape[0] // 2
        blocks = lambda ref: lambda origin: ref.at[origin]
        part = lambda ref, i: lambda origin: ref.at[origin, pl.ds(i * half, half)]
        weights = DpGather(at, [None, None, wd_ref.at[pl.ds(0, half)], wg_ref, wu_ref], [*map(blocks, (wqkv_s, wo_s)), part(d_out, 0), *map(blocks, (g_out, u_out))],
                           ds, dr, dl)
        other = DpSides(at, wd_ref.at[pl.ds(half, half)], part(d_out, 1), es, er, el)
        qkv, last, down, gate, up = range(5)
        states = [TpGather(at, s, o, ts.at[n], tr.at[n], tl.at[n]) for n, (s, o) in enumerate(((None, a_s), (dy_ref, dy_out), (b_s, b_out)))]
        weights.launch(qkv, 0)
        weights.launch(last, 0)
        states[0].start()
        states[1].start()

        def table(i, _):
            rows = 256
            here = pl.ds(pl.multiple_of(i * rows, rows), rows)
            lane = lax.broadcasted_iota(jnp.int32, (rows, HEAD), 1)
            token = (lax.broadcasted_iota(jnp.int32, (rows, HEAD), 0) + i * rows).astype(F32)
            low = lane < HALF
            angle = token * jnp.exp((jnp.where(low, lane, lane - HALF).astype(F32)) * (-jnp.log(jnp.float32(THETA)) / HALF))
            cos_ref[here, :] = jnp.cos(angle)
            sine = jnp.sin(angle)
            sin_ref[here, :] = jnp.where(low, -sine, sine)

        lax.fori_loop(0, TOKENS // 256, table, None)
        gap_s[:] = _gap((B, B))
        for r in (1, 2):
            weights.next(qkv, r)
            weights.next(last, r)
        states[0].middle()
        weights.next(qkv, 3)
        weights.next(last, 3)
        weights.launch(down, 0)
        other.start()
        weights.launch(gate, 0)
        other.launch(0, 0)
        states[0].finish()
        for r in range(4):
            weights.close(qkv, r)

        def project(t, _):
            here = _block(t)
            c, s = cos_ref[here, :], sin_ref[here, :]
            for i, ref in enumerate((q_ref, k_ref, v_ref)):
                all_heads = _mm(a_s[t], wqkv_s[:, i].reshape(B, B)).astype(BF)
                for h, one in enumerate(_heads(all_heads)):
                    ref[h, here, :] = one if ref is v_ref else _turn(one.astype(F32), c, s).astype(BF)

        lax.fori_loop(0, TOKENS // B, project, None)
        for r in range(4):
            weights.close(last, r)
        sums = TpReduce(at, *reduce)

        def tile(n, _):
            t = sums.block(n)
            here = _block(t)
            top_s[:] = jnp.full_like(top_s, NEG)
            mix_s[:] = jnp.zeros_like(mix_s)
            ones = jnp.ones((8, B), BF)

            @pl.when(n == 0)
            def _():
                weights.next(down, 1)
                other.launch(1, 0)

            @pl.when(n == 1)
            def _():
                states[1].middle()
                weights.next(gate, 1)
                other.launch(0, 1)

            @pl.when(n == 2)
            def _():
                weights.next(down, 2)
                other.launch(1, 1)

            @pl.when(n == 3)
            def _():
                weights.next(gate, 2)
                other.launch(0, 2)
                weights.launch(up, 0)

            def block(j, masked):
                keys = _block(j)
                scores = [_mt(k_ref[h, keys, :], q_ref[h, here, :]) for h in range(HEADS)]
                weigh, keep = [], []
                for h, sc in enumerate(scores):
                    if masked:
                        sc = jnp.where(gap_s[:] >= 0, sc, HIDDEN)
                    one = slice(h, h + 1)
                    old = top_s[one, :]
                    top = jnp.maximum(old, sc.max(axis=0, keepdims=True))
                    top_s[one, :] = top
                    weigh.append(jnp.exp2((sc - top) * e).astype(BF))
                    keep.append(jnp.exp2((old - top) * e))
                for h in range(HEADS):
                    values = jnp.concatenate([v_ref[h, keys, :].T, ones], axis=0)
                    mix_s[h] = mix_s[h] * keep[h] + _mm(values, weigh[h])

            lax.fori_loop(0, t, lambda j, _: block(j, False), None)
            block(t, True)
            for h in range(HEADS):
                one = slice(h, h + 1)
                total = mix_s[h, HEAD : HEAD + 1, :]
                o_ref[h, here, :] = (mix_s[h, :HEAD, :] * (1 / total)).T.astype(BF)
                lse_ref[one, here] = top_s[one, :] * SCALE + jnp.log(total)

            mixed = jnp.concatenate([o_ref[h, here, :] for h in range(HEADS)], axis=1)
            sums.add(n, _mm(mixed, wo_s[:].reshape(B, B)))

        lax.fori_loop(0, TOKENS // B, tile, None)
        weights.next(down, 3)
        other.launch(1, 2)
        weights.next(gate, 3)
        keep = ((q_ref, q_out), (k_ref, k_out), (v_ref, v_out), (o_ref, o_out), (a_s, a_out), (wqkv_s, wqkv_out), (wo_s, wo_out))
        keep = [pltpu.make_async_copy(s, o, ls.at[n]) for n, (s, o) in enumerate(keep)]
        for c in keep:
            c.start()
        h = (x_ref[:].astype(F32) + _round(sums.total())).astype(BF)
        h_ref[:] = h
        b_s[:] = _normed(h.astype(F32)).astype(BF)
        states[2].start()
        for r in range(1, 4):
            weights.next(up, r)
        states[2].middle()
        states[1].finish()
        states[2].finish()
        for n in (down, gate, up):
            for r in range(4):
                weights.close(n, r)
        other.close()
        for c in keep:
            c.wait()

    wqkv, last = (8, 3, *wq.shape), (8, *wo.shape)
    outs = [BLOCK, STATES, STATES, STATES, _shape(wqkv), _shape(last), *[_shape((8, *w.shape)) for w in (wg, wu, wd)], *[PER_HEAD] * 4,
            _shape((HEADS, TOKENS), F32), *[_shape((TOKENS, HEAD), F32)] * 2]
    scratch = [pltpu.VMEM((4, B, B), BF), pltpu.VMEM((B, B), BF), pltpu.VMEM(wqkv, BF), pltpu.VMEM(last, BF), *[pltpu.VMEM(PER_HEAD.shape, BF)] * 4,
               pltpu.VMEM((HEADS, B), F32), pltpu.VMEM((HEADS, HEAD + 8, B), F32), pltpu.VMEM((B, B), jnp.int32),
               *_sems((3, 3), (3, 3), (3,), (5, MOVES), (5, MOVES), (5,), (MOVES,), (MOVES,), (), (7,)), *_tp_scratch()]
    return _comm(kernel, "forward", 0, (x, dy, wq, wk, wv, wo, wg, wu, wd), outs, [INV] + [ANY] * 12 + [INV] * 3, scratch, [INV] * 9)


def _ffn(b, dy, g, u, d, h):
    chunks, per = FF // WIDE, WIDE // 256

    def kernel(b_any, dy_any, g_ref, u_ref, d_ref, h_ref, dh_ref, dh_out, dg_out, du_out, dd_out, early_out,
               b_ref, dy_ref, g_s, u_s, d_s, dgate_s, dup_s, hidden_s, bt_s, dyt_s, wdt_s, wgut_s, db_s, ls, gs, gr, gl, ys, yr, *reduce):
        at = Place()
        loads = [pltpu.make_async_copy(s, o, ls.at[n]) for n, (s, o) in enumerate(((g_ref, g_s), (u_ref, u_s), (d_ref, d_s), (b_any, b_ref), (dy_any, dy_ref)))]
        for c in loads:
            c.start()
        at.meet(True, True)
        for c in loads:
            c.wait()
        sums = TpReduce(at, *reduce)

        def columns(j):
            return pl.ds(j * WIDE, WIDE) if isinstance(j, int) else pl.ds(pl.multiple_of(j * WIDE, WIDE), WIDE)

        def prepare(j, _):
            c = columns(j)
            wdt_s[:, c] = d_s[pl.ds(j * per, per)].reshape(WIDE, B).T
            wgut_s[j, :WIDE] = g_s[:, :, c].reshape(B, WIDE).T
            wgut_s[j, WIDE:] = u_s[:, :, c].reshape(B, WIDE).T

        lax.fori_loop(0, chunks, prepare, None)

        def tile(k, _):
            t = sums.block(k)
            rows = _block(t)
            b, dy = b_ref[t], dy_ref[t]
            bt_s[:, rows] = b.T
            dyt_s[:, rows] = dy.T
            db_s[:] = jnp.zeros_like(db_s)

            def hidden(j):
                c = columns(j)
                gate = _mm(b, g_s[:, :, c].reshape(B, WIDE))
                up = _mm(b, u_s[:, :, c].reshape(B, WIDE))
                dh = _round(_mm(dy, wdt_s[:, c]))
                sig = jax.nn.sigmoid(gate)
                act = gate * sig
                dup = (dh * act).astype(BF)
                dgate = (dh * up * (sig + act * (1 - sig))).astype(BF)
                hidden_s[rows, c] = (act * up).astype(BF)
                dup_s[rows, c] = dup
                dgate_s[rows, c] = dgate

            def states(j):
                c = columns(j)
                db_s[:] += _mm(jnp.concatenate([dgate_s[rows, c], dup_s[rows, c]], axis=1), wgut_s[j])

            hidden(0)
            for j in range(1, chunks):
                hidden(j)
                states(j - 1)
            states(chunks - 1)
            sums.add(k, db_s[:])

        lax.fori_loop(0, TOKENS // B, tile, None)
        back = _normed_bwd(h_ref[:].astype(F32), _round(sums.total()))
        dh_ref[:] = (dy_ref[at.tp].astype(F32) + _round(back)).astype(BF)
        states = TpGather(at, dh_ref, dh_out, gs, gr, gl)
        states.start()

        def down(i, _):
            j = lax.rem(i + lax.div(at.other_row, 2), 4)
            d_s[pl.ds(2 * j, 2)] = _mm(dyt_s[:], hidden_s[:, _block(j)]).T.astype(BF).reshape(2, B // 2, B)

        lax.fori_loop(0, 2, down, None)
        stores = [pltpu.make_async_copy(s, o, ls.at[n]) for n, (s, o) in enumerate(((g_s, dg_out), (u_s, du_out), (d_s, dd_out)))]

        def across(z):
            return [_send(d_s.at[at.other_row + d], early_out.at[d], ys.at[i], yr.at[i], at.to_y) for i, d in enumerate(ORDER[z][:EARLY])]

        for z in range(4):

            @pl.when(at.z == z)
            def _():
                for c in across(z):
                    c.start()

        lax.fori_loop(2, 4, down, None)
        stores[2].start()
        for term, out in ((dgate_s, g_s), (dup_s, u_s)):

            def gate_up(j, _):
                out[:, :, _block(j)] = _mm(bt_s[:], term[:, _block(j)]).astype(BF).reshape(8, B // 8, B)

            lax.fori_loop(0, FF // B, gate_up, None)
            if out is g_s:
                stores[0].start()
                states.middle()
        stores[1].start()
        states.finish()
        for z in range(4):

            @pl.when(at.z == z)
            def _():
                for c in across(z):
                    c.wait()

        for c in stores:
            c.wait()

    wide, tall, big = pltpu.VMEM((B, FF), BF), pltpu.VMEM(g.shape, BF), pltpu.VMEM((TOKENS, FF), BF)
    scratch = [pltpu.VMEM(b.shape, BF), pltpu.VMEM(b.shape, BF), tall, tall, pltpu.VMEM(d.shape, BF), big, big, big, wide, wide, wide, pltpu.VMEM((chunks, 2 * WIDE, B), BF), pltpu.VMEM((B, B), F32),
               *_sems((5,), (3,), (3,), (), (EARLY,), (EARLY,)), *_tp_scratch()]
    outs = [BLOCK, STATES, _shape(g.shape), _shape(u.shape), _shape(d.shape), _shape((4, *d.shape[1:]))]
    return _comm(kernel, "ffn", 3, (b, dy, g, u, d, h), outs, [INV] + [ANY] * 5, scratch, [ANY] * 5 + [INV])


def _back(dh, a, wqkv, wo, cos, sin, q, k, v, heads, lse, early, parts):
    e = SCALE * LOG2E
    count = len(parts)

    def kernel(*refs):
        given, (early_ref, *refs) = refs[: len(held)], refs[len(held) :]
        parts_ref, (da_ref, dwq_ref, dwk_ref, dwv_ref, dwo_out, early_out, *refs) = refs[:count], refs[count:]
        outs, (hs, dwo_s, ws, wr, wl, *refs) = refs[:count], refs[count:]
        here, (do_s, dq_s, dk_s, dv_s, gap_s, acc_s, *refs) = refs[: len(held)], refs[len(held) :]
        dh_s, a_ref, wqkv_ref, wo_ref, cos_ref, sin_ref, q_ref, k_ref, v_ref, o_ref, lse_ref = here
        loads = [pltpu.make_async_copy(s, o, hs.at[n]) for n, (s, o) in enumerate(zip(given, here))]
        scratch, (ds, dr, dl) = refs[: 4 * count], refs[4 * count :]
        at = Place()
        at.meet(True, False)
        sums = DpReduce(at, parts_ref, [scratch[4 * n : 4 * n + 4] for n in range(count)], ds, dr, dl, early_ref, EARLY)
        sums.start()
        for c in loads:
            c.start()
        gap_s[:] = _gap((B, B))
        acc_s[:] = jnp.zeros_like(acc_s)
        dk_s[:] = jnp.zeros_like(dk_s)
        dv_s[:] = jnp.zeros_like(dv_s)
        sums.ready()
        sums.stage(0, 0)
        for c in loads:
            c.wait()
        mixed = [jnp.concatenate([o_ref[h, _block(t), :] for h in range(HEADS)], axis=1) for t in range(4)]
        dwo_s[:] = sum(_tm(m, dh_s[t]) for t, m in enumerate(mixed)).astype(BF).reshape(dwo_s.shape)
        mix_store = pltpu.make_async_copy(dwo_s, dwo_out, wl)
        mix_store.start()
        mix_sends = [_send(dwo_s.at[at.other_row + d], early_out.at[d], ws.at[d], wr.at[d], at.to_y) for d in range(4)]
        for c in mix_sends:
            c.start()

        def tile(i, _):
            t = 3 - i
            here = _block(t)


            @pl.when(i == 1)
            def _():
                sums.stage(0, 2)
                sums.stage(1, 1)

            pl.when(i == 2)(lambda: sums.stage(1, 2))
            pl.when(i == 3)(lambda: sums.stage(2, 2))
            dh = dh_s[t]
            mixed = [o_ref[h, here, :] for h in range(HEADS)]
            do_s[:] = _mt(dh, wo_ref[:].reshape(B, B)).astype(BF)
            dos = _heads(do_s)
            deltas = [(x.astype(F32) * y.astype(F32)).T.sum(axis=0, keepdims=True) for x, y in zip(dos, mixed)]
            lses = [lse_ref[h : h + 1, here] * LOG2E for h in range(HEADS)]
            dq_s[:] = jnp.zeros_like(dq_s)

            def block(j, masked):
                keys = _block(j)
                scores = [_mt(k_ref[h, keys, :], q_ref[h, here, :]) for h in range(HEADS)]
                dps = [_mt(v_ref[h, keys, :], do_s[:, h * HEAD : (h + 1) * HEAD]) for h in range(HEADS)]
                for h in range(HEADS):
                    p = jnp.exp2(scores[h] * e - lses[h])
                    if masked:
                        p = jnp.where(gap_s[:] >= 0, p, 0.0)
                    ds = (p * (dps[h] - deltas[h])).astype(BF)
                    dv_s[h, keys, :] += _mm(p.astype(BF), do_s[:, h * HEAD : (h + 1) * HEAD])
                    dk_s[h, keys, :] += _mm(ds, q_ref[h, here, :])
                    dq_s[h] += _mm(k_ref[h, keys, :].T, ds)

            def whole(j, _):
                @pl.when(jnp.logical_and(i == 0, j == 1))
                def _():
                    sums.stage(0, 1)
                    sums.stage(1, 0)

                pl.when(jnp.logical_and(i == 0, j == 2))(lambda: sums.stage(2, 0))
                pl.when(jnp.logical_and(i == 1, j == 1))(lambda: sums.stage(2, 1))
                block(j, False)

            lax.fori_loop(0, t, whole, None)
            block(t, True)
            c, s = cos_ref[here, :], -sin_ref[here, :]
            da = jnp.zeros((B, B), F32)
            for n, ref in enumerate((dq_s, dk_s, dv_s)):
                g = []
                for h in range(HEADS):
                    one = dq_s[h].T if ref is dq_s else ref[h, here, :]
                    g.append(one.astype(BF) if ref is dv_s else _turn(_round(one * SCALE), c, s).astype(BF))
                g = jnp.concatenate(g, axis=1)
                da += _mt(g, wqkv_ref[:, n].reshape(B, B))
                acc_s[n] += _tm(a_ref[t], g)
            da_ref[t] = da.astype(BF)

        lax.fori_loop(0, TOKENS // B, tile, None)
        for n, ref in enumerate((dwq_ref, dwk_ref, dwv_ref)):
            ref[:] = acc_s[n].astype(BF)
        sums.finish(outs)
        mix_store.wait()
        for c in mix_sends:
            c.wait()

    held = (dh, a, wqkv, wo, cos, sin, q, k, v, heads, lse)
    blocks = [p.shape[1:] for p in parts]
    scratch = [*_sems((len(held),)), pltpu.VMEM(wo.shape, BF), *_sems((4,), (4,), ()), *[pltpu.VMEM(t.shape, t.dtype) for t in held], pltpu.VMEM((B, B), BF), pltpu.VMEM((HEADS, HEAD, B), F32), pltpu.VMEM(PER_HEAD.shape, F32), pltpu.VMEM(PER_HEAD.shape, F32),
               pltpu.VMEM((B, B), jnp.int32), pltpu.VMEM((3, B, B), F32), *_reduce_scratch(blocks), *_reduce_sems(count)]
    return _comm(kernel, "back", 4, (*held, early, *parts), [STATES, *[BLOCK] * 3, _shape(wo.shape), _shape((4, *wo.shape[1:])), *map(_shape, blocks)], [INV] * 4 + [ANY] * 2 + [INV] * count, scratch,
                 [ANY] * (len(held) + 1 + count))


def _finish(da, x, dh, early, parts):
    count = len(parts)

    def kernel(da_ref, x_ref, dh_ref, early_ref, *refs):
        parts_ref, (dx_ref, *refs) = refs[:count], refs[count:]
        outs, (*refs, ds, dr, dl) = refs[:count], refs[count:]
        tp = len(refs) - 4 * count
        reduce, scratch = refs[:tp], refs[tp:]
        at = Place()
        at.meet(True, True)
        weights = DpReduce(at, parts_ref, [scratch[4 * n : 4 * n + 4] for n in range(count)], ds, dr, dl, early_ref, 4)
        weights.start()
        weights.ready()
        weights.stage(0, 0)
        sums = TpReduce(at, *reduce)
        for k in range(4):
            sums.add(k, da_ref[sums.block(k)].astype(F32))
        for s in range(3):
            for n in range(count):
                if s + n > 0:
                    weights.stage(n, s)
        back = _normed_bwd(x_ref[:].astype(F32), _round(sums.total()))
        dx_ref[:] = (dh_ref[:].astype(F32) + _round(back)).astype(BF)
        weights.finish(outs)

    blocks = [p.shape[1:] for p in parts]
    scratch = [*_tp_scratch(), *_reduce_scratch(blocks), *_reduce_sems(count)]
    return _comm(kernel, "finish", 5, (da, x, dh, early, *parts), [BLOCK, *map(_shape, blocks)], [INV] * (1 + count), scratch, [INV] * 3 + [ANY] * (1 + count))


def _copies(arrays):
    count = len(arrays)

    def kernel(*refs):
        for a, b in zip(refs[:count], refs[count:]):
            b[:] = a[:]

    return pl.pallas_call(kernel, name="copies", out_shape=[_shape(a.shape) for a in arrays], in_specs=[INV] * count, out_specs=[INV] * count)(*arrays)


def solution(mesh):
    def step(x, dy, wq, wk, wv, wo, wg, wu, wd):
        x, dy = x[0], dy[0]
        h, b, a, all_dy, wqkv, wo, g, u, d, q, k, v, heads, lse, cos, sin = _forward(x, dy, wq, wk, wv, wo, wg, wu, wd)
        dh, all_dh, dg, du, dd, early = _ffn(b, all_dy, g, u, d, h)
        da, dwq, dwk, dwv, dwo, early, *more = _back(all_dh, a, wqkv, wo, cos, sin, q, k, v, heads, lse, early, (dd, dg, du))
        parts = [dwo, *[w.reshape(wo.shape) for w in (dwq, dwk, dwv)]]
        dx, dwo, dwq, dwk, dwv, dd, dg, du = _copies([*_finish(da, x, dh, early, parts), *more])
        return dx[None], dwq, dwk, dwv, dwo, dg, du, dd

    states, by_columns, by_rows = P("dp", "tp", None), P("dp", "tp"), P(("tp", "dp"), None)
    weights = (by_columns, by_columns, by_columns, by_rows, by_columns, by_columns, by_rows)
    return jax.shard_map(step, mesh=mesh, in_specs=(states, states, *weights), out_specs=(states, *weights), check_vma=False)
```

```python
import functools

import jax
import jax.numpy as jnp
from jax import lax
from jax.experimental import pallas as pl
from jax.experimental.pallas import tpu as pltpu
from jax.sharding import PartitionSpec as P

HEADS, HEAD, THETA = 4, 128, 10000
HALF = HEAD // 2
B = 512
TOKENS, FF, WIDE = 2048, 2048, 256
NEG, HIDDEN = -1e30, -2e30
LOG2E = 1.4426950408889634
SCALE = HEAD**-0.5
F32, BF = jnp.float32, jnp.bfloat16
MESH = pl.DeviceIdType.MESH
ROOM = 67043328
ANY = pl.BlockSpec(memory_space=pl.ANY)
INV = pl.BlockSpec(memory_space=pltpu.VMEM)
EARLY = 4
RIGHT, LEFT, Y, YL, YR, MOVES = 0, 3, 6, 7, 10, 13


def _dot(a, b, ca, cb):
    return lax.dot_general(a, b, (((ca,), (cb,)), ((), ())), preferred_element_type=F32)


def _mm(a, b):
    return _dot(a, b, 1, 0)


def _mt(a, b):
    return _dot(a, b, 1, 1)


def _tm(a, b):
    return _dot(a, b, 0, 0)


def _normed(wide):
    return wide * lax.rsqrt(jnp.mean(wide * wide, -1, keepdims=True) + 1e-6)


def _normed_bwd(wide, g):
    r = lax.rsqrt(jnp.mean(wide * wide, -1, keepdims=True) + 1e-6)
    return g * r - wide * (r * r * r * jnp.mean(g * wide, -1, keepdims=True))


def _round(t):
    return t.astype(BF).astype(F32)


def _block(i):
    return pl.ds(pl.multiple_of(i * B, B), B)


def _send(src, dst, ss, rs, where):
    return pltpu.make_async_remote_copy(src_ref=src, dst_ref=dst, send_sem=ss, recv_sem=rs, device_id=where, device_id_type=MESH)


class Place:
    def __init__(self):
        self.dp, self.tp = lax.axis_index("dp"), lax.axis_index("tp")
        self.z, self.y = lax.rem(self.dp, 4), lax.div(self.dp, 4)
        self.row = self.y * 4
        self.other_row = 4 - self.row
        self.across = lax.rem(self.tp + 2, 4)
        self.core = self.tp + 1 - 2 * lax.rem(self.tp, 2)
        self.diagonal = 3 - self.tp
        self.to_y = {"dp": self.other_row + self.z, "tp": self.tp}
        self.to_right = {"dp": self.dp + 1, "tp": self.tp}
        self.to_left = {"dp": self.dp - 1, "tp": self.tp}
        self.to_across = {"dp": self.dp, "tp": self.across}
        self.to_core = {"dp": self.dp, "tp": self.core}

    def meet(self, dp, tp):
        bar = pltpu.get_barrier_semaphore()
        tell = lambda where: pl.semaphore_signal(bar, inc=1, device_id=where, device_id_type=MESH)
        count = 0
        if tp:
            tell(self.to_across)
            tell(self.to_core)
            count += 2
        if dp:
            tell(self.to_y)
            count += 1

            @pl.when(self.z > 0)
            def _():
                tell(self.to_left)

            @pl.when(self.z < 3)
            def _():
                tell(self.to_right)

            count += 1 + lax.div(self.z * (3 - self.z) + 1, 2)

        pl.semaphore_wait(bar, count)


class TpGather:
    def __init__(self, at, src, out, ss, rs, ls):
        self.own = None if src is None else pltpu.make_async_copy(src, out.at[at.tp], ls)
        src = out.at[at.tp] if src is None else src
        self.a = _send(src, out.at[at.tp], ss.at[0], rs.at[0], at.to_across)
        self.c = _send(src, out.at[at.tp], ss.at[1], rs.at[1], at.to_core)
        self.f = _send(out.at[at.across], out.at[at.across], ss.at[2], rs.at[2], at.to_core)

    def start(self):
        self.a.start()
        self.c.start()
        if self.own is not None:
            self.own.start()

    def middle(self):
        self.a.wait_recv()
        self.f.start()

    def finish(self):
        self.c.wait_recv()
        self.f.wait_recv()
        self.a.wait_send()
        self.c.wait_send()
        self.f.wait_send()
        if self.own is not None:
            self.own.wait()


class DpGather:
    def __init__(self, at, srcs, outs, ss, rs, ls):
        self.at, self.srcs, self.outs, self.ss, self.rs, self.ls = at, srcs, outs, ss, rs, ls

    def move(self, n, i, first, origin, where):
        to = self.outs[n](origin)
        src = self.srcs[n] if first and self.srcs[n] is not None else to
        return _send(src, to, self.ss.at[n, i], self.rs.at[n, i], where)

    def lines(self, n, s):
        at, first = self.at, s == 0
        yield (self.move(n, RIGHT + s, first, at.dp - s, at.to_right), jnp.logical_and(at.z >= s, at.z < 3),
               self.move(n, RIGHT + s, False, at.dp - 1 - s, at.to_right), at.z > s)
        yield (self.move(n, LEFT + s, first, at.dp + s, at.to_left), jnp.logical_and(at.z + s <= 3, at.z > 0),
               self.move(n, LEFT + s, False, at.dp + 1 + s, at.to_left), at.z + s < 3)

    def sides(self, n, r):
        at = self.at
        if r == 0:
            yield self.move(n, Y, True, at.dp, at.to_y), at.z >= 0
        else:
            yield self.move(n, YL + r - 1, False, at.dp - r, at.to_y), at.z >= r
            yield self.move(n, YR + r - 1, False, at.dp + r, at.to_y), at.z + r <= 3

    def local(self, n):
        return pltpu.make_async_copy(self.srcs[n], self.outs[n](self.at.dp), self.ls.at[n])

    def launch(self, n, r):
        if r < 3:
            for out, sends, _, _ in self.lines(n, r):
                pl.when(sends)(out.start)
        for out, sends in self.sides(n, r):
            pl.when(sends)(out.start)
        if r == 0 and self.srcs[n] is not None:
            self.local(n).start()

    def arrive(self, n, r):
        for _, _, got, comes in self.lines(n, r):
            pl.when(comes)(got.wait_recv)

    def close(self, n, r):
        if r < 3:
            for out, sends, _, _ in self.lines(n, r):
                pl.when(sends)(out.wait_send)
        for out, sends in self.sides(n, r):
            pl.when(sends)(out.wait)
        if r == 0 and self.srcs[n] is not None:
            self.local(n).wait()

    def next(self, n, r):
        self.arrive(n, r - 1)
        self.launch(n, r)


class DpSides:
    def __init__(self, at, src, out, ss, rs, ls):
        self.at, self.src, self.out, self.ss, self.rs = at, src, out, ss, rs
        self.y = _send(src, out(at.dp), ss.at[Y], rs.at[Y], at.to_y)
        self.own = pltpu.make_async_copy(src, out(at.dp), ls)

    def start(self):
        self.y.start()
        self.own.start()

    def lines(self, row, s):
        at = self.at
        first = row == 0
        base = at.dp if first else at.other_row + at.z
        numbers = (RIGHT, LEFT) if first else (YL, YR)
        for i, step, sends, comes in ((numbers[0], -1, jnp.logical_and(at.z >= s, at.z < 3), at.z > s),
                                      (numbers[1], 1, jnp.logical_and(at.z + s <= 3, at.z > 0), at.z + s < 3)):
            to = at.to_right if step < 0 else at.to_left
            out, came = self.out(base + step * s), self.out(base + step * (s + 1))
            src = self.src if first and s == 0 else out
            yield (_send(src, out, self.ss.at[i + s], self.rs.at[i + s], to), sends, _send(came, came, self.ss.at[i + s], self.rs.at[i + s], to), comes)

    def launch(self, row, s):
        if s == 0 and row == 1:
            self.y.wait_recv()
        if s > 0:
            self.arrive(row, s - 1)
        for out, sends, _, _ in self.lines(row, s):
            pl.when(sends)(out.start)

    def arrive(self, row, s):
        for _, _, got, comes in self.lines(row, s):
            pl.when(comes)(got.wait_recv)

    def close(self):
        for row in range(2):
            self.arrive(row, 2)
            for s in range(3):
                for out, sends, _, _ in self.lines(row, s):
                    pl.when(sends)(out.wait_send)
        self.y.wait_send()
        self.own.wait()


ORDER = ((3, 2, 1, 0), (3, 0, 2, 1), (0, 3, 1, 2), (0, 1, 2, 3))


class DpReduce:
    def __init__(self, at, parts, scratch, ss, rs, ls, early, count):
        self.at, self.parts, self.ss, self.rs, self.ls = at, parts, ss, rs, ls
        self.scratch, self.early, self.count = scratch, early, count

    def local(self, n):
        return pltpu.make_async_copy(self.parts[n].at[pl.ds(self.at.row, 4)], self.scratch[n][0], self.ls.at[n])

    def across(self, n, d):
        return _send(self.parts[n].at[self.at.other_row + d], self.scratch[n][1].at[d], self.ss.at[n, d], self.rs.at[n, d], self.at.to_y)

    def go_right(self, n, s, d):
        i = 4 + s
        return _send(self.scratch[n][0].at[d], self.scratch[n][2].at[s], self.ss.at[n, i], self.rs.at[n, i], self.at.to_right)

    def go_left(self, n, s, d):
        i = 7 + s
        return _send(self.scratch[n][0].at[d], self.scratch[n][3].at[s], self.ss.at[n, i], self.rs.at[n, i], self.at.to_left)

    def came(self, n, i):
        return n == 0 and i < self.count

    def each(self, body):
        for z in range(4):
            pl.when(self.at.z == z)(functools.partial(body, z))

    def start(self):
        for n in range(len(self.parts)):
            self.local(n).start()

        def go(z):
            for i, d in enumerate(ORDER[z]):
                for n in range(len(self.parts)):
                    if self.came(n, i):
                        pltpu.make_async_copy(self.early.at[d], self.scratch[n][1].at[d], self.rs.at[n, d]).start()
                    else:
                        self.across(n, d).start()

        self.each(go)

    def ready(self):
        for n in range(len(self.parts)):
            self.local(n).wait()

    def total(self, n, z, d, s, left, right, out):
        mine, got_y, from_left, from_right = self.scratch[n]
        if self.came(n, ORDER[z].index(d)):
            pltpu.make_async_copy(self.early.at[d], got_y.at[d], self.rs.at[n, d]).wait()
        else:
            self.across(n, d).wait_recv()
        terms = [mine.at[d], got_y.at[d]]
        if left:
            self.go_right(n, s, z).wait_recv()
            terms.append(from_left.at[s])
        if right:
            self.go_left(n, s, z).wait_recv()
            terms.append(from_right.at[s])
        size = mine.shape[1] // 4

        def rows(i, _):
            here = pl.ds(pl.multiple_of(i * size, size), size)
            out[here, :] = sum(t[here, :].astype(F32) for t in terms).astype(BF)

        lax.fori_loop(0, 4, rows, None)

    def stage(self, n, s):
        def go(z):
            mine = self.scratch[n][0]
            if z <= s and z < 3:
                d = 3 - s + z
                self.total(n, z, d, s - 1, z > 0, False, mine.at[d])
                self.go_right(n, s, d).start()
            if z + s >= 3 and z > 0:
                d = s - 3 + z
                self.total(n, z, d, s - 1, False, z < 3, mine.at[d])
                self.go_left(n, s, d).start()

        self.each(go)

    def finish(self, outs):
        def go(z):
            for n, out in enumerate(outs):
                self.total(n, z, z, 2, z > 0, z < 3, out)
                for i, d in enumerate(ORDER[z]):
                    if not self.came(n, i):
                        self.across(n, d).wait_send()
                for s in range(3):
                    if z <= s and z < 3:
                        self.go_right(n, s, z).wait_send()
                    if z + s >= 3 and z > 0:
                        self.go_left(n, s, z).wait_send()

        self.each(go)


def _reduce_scratch(shapes):
    return [pltpu.VMEM((k, *s), BF) for s in shapes for k in (4, 4, 3, 3)]


def _reduce_sems(count):
    return _sems((count, 10), (count, 10), (count,))


class TpReduce:
    def __init__(self, at, to_c, from_c, to_a, from_a, near, ss, rs):
        self.at, self.to_c, self.from_c, self.to_a, self.from_a, self.near = at, to_c, from_c, to_a, from_a, near
        self.c = [_send(to_c.at[i], from_c.at[i], ss.at[i], rs.at[i], at.to_core) for i in range(2)]
        self.a = _send(to_a, from_a, ss.at[2], rs.at[2], at.to_across)

    def block(self, k):
        x, core = lax.div(self.at.tp, 2), lax.rem(self.at.tp, 2)
        other_x, other_core = 1 - lax.div(k, 2), 1 - lax.rem(k, 2)
        return 2 * (x + (1 - 2 * x) * other_x) + core + (1 - 2 * core) * other_core

    def add(self, k, term):
        for i in range(2):

            @pl.when(k == 2 * i)
            def _():
                self.to_c[i] = term.astype(BF)
                self.c[i].start()

        @pl.when(k == 1)
        def _():
            self.c[0].wait_recv()
            self.to_a[:] = (term + self.from_c[0].astype(F32)).astype(BF)
            self.a.start()

        @pl.when(k == 3)
        def _():
            self.c[1].wait_recv()
            self.near[:] = term + self.from_c[1].astype(F32)

    def total(self):
        self.a.wait()
        for c in self.c:
            c.wait_send()
        return self.near[:] + self.from_a[:].astype(F32)


def _tp_scratch():
    one, two = (B, B), (2, B, B)
    return [pltpu.VMEM(two, BF), pltpu.VMEM(two, BF), pltpu.VMEM(one, BF), pltpu.VMEM(one, BF), pltpu.VMEM(one, F32), *_sems((3,), (3,))]


def _sems(*shapes):
    return [pltpu.SemaphoreType.DMA(s) for s in shapes]


def _shape(shape, dtype=BF):
    return jax.ShapeDtypeStruct(shape, dtype)


BLOCK, STATES = _shape((B, B)), _shape((4, B, B))
PER_HEAD = _shape((HEADS, TOKENS, HEAD))


def _comm(kernel, name, number, ins, outs, out_specs, scratch, in_specs, aliases={}):
    return pl.pallas_call(
        kernel, name=name, out_shape=outs, in_specs=in_specs, out_specs=out_specs, scratch_shapes=scratch, input_output_aliases=aliases,
        compiler_params=pltpu.CompilerParams(collective_id=number, has_side_effects=True, vmem_limit_bytes=ROOM),
    )(*ins)


def _turn(t, cos, sin):
    return t * cos + pltpu.roll(t, HALF, 1) * sin


def _gap(shape):
    return lax.broadcasted_iota(jnp.int32, shape, 1) - lax.broadcasted_iota(jnp.int32, shape, 0)


def _heads(t):
    return [t[:, h * HEAD : (h + 1) * HEAD] for h in range(HEADS)]


def _forward(x, dy, wq, wk, wv, wo, wg, wu, wd):
    e = SCALE * LOG2E

    def kernel(x_ref, dy_ref, wq_ref, wk_ref, wv_ref, wo_ref, wg_ref, wu_ref, wd_ref,
               h_ref, b_out, a_out, dy_out, wqkv_out, wo_out, g_out, u_out, d_out, q_out, k_out, v_out, o_out, lse_ref, cos_ref, sin_ref,
               a_s, b_s, wqkv_s, wo_s, q_ref, k_ref, v_ref, o_ref, top_s, mix_s, gap_s, ts, tr, tl, ds, dr, dl, es, er, el, ls, *reduce):
        at = Place()
        for i, w in enumerate((wq_ref, wk_ref, wv_ref)):
            wqkv_s[at.dp, i] = w[:]
        wo_s[at.dp] = wo_ref[:]
        a_s[at.tp] = _normed(x_ref[:].astype(F32)).astype(BF)
        at.meet(True, True)
        half = wd_ref.shape[0] // 2
        blocks = lambda ref: lambda origin: ref.at[origin]
        part = lambda ref, i: lambda origin: ref.at[origin, pl.ds(i * half, half)]
        weights = DpGather(at, [None, None, wd_ref.at[pl.ds(0, half)], wg_ref, wu_ref], [*map(blocks, (wqkv_s, wo_s)), part(d_out, 0), *map(blocks, (g_out, u_out))],
                           ds, dr, dl)
        other = DpSides(at, wd_ref.at[pl.ds(half, half)], part(d_out, 1), es, er, el)
        qkv, last, down, gate, up = range(5)
        states = [TpGather(at, s, o, ts.at[n], tr.at[n], tl.at[n]) for n, (s, o) in enumerate(((None, a_s), (dy_ref, dy_out), (b_s, b_out)))]
        weights.launch(qkv, 0)
        weights.launch(last, 0)
        states[0].start()
        states[1].start()

        def table(i, _):
            rows = 256
            here = pl.ds(pl.multiple_of(i * rows, rows), rows)
            lane = lax.broadcasted_iota(jnp.int32, (rows, HEAD), 1)
            token = (lax.broadcasted_iota(jnp.int32, (rows, HEAD), 0) + i * rows).astype(F32)
            low = lane < HALF
            angle = token * jnp.exp((jnp.where(low, lane, lane - HALF).astype(F32)) * (-jnp.log(jnp.float32(THETA)) / HALF))
            cos_ref[here, :] = jnp.cos(angle)
            sine = jnp.sin(angle)
            sin_ref[here, :] = jnp.where(low, -sine, sine)

        lax.fori_loop(0, TOKENS // 256, table, None)
        gap_s[:] = _gap((B, B))
        for r in (1, 2):
            weights.next(qkv, r)
            weights.next(last, r)
        states[0].middle()
        weights.next(qkv, 3)
        weights.next(last, 3)
        weights.launch(down, 0)
        other.start()
        weights.launch(gate, 0)
        other.launch(0, 0)
        states[0].finish()
        for r in range(4):
            weights.close(qkv, r)

        def project(t, _):
            here = _block(t)
            c, s = cos_ref[here, :], sin_ref[here, :]
            for i, ref in enumerate((q_ref, k_ref, v_ref)):
                all_heads = _mm(a_s[t], wqkv_s[:, i].reshape(B, B)).astype(BF)
                for h, one in enumerate(_heads(all_heads)):
                    ref[h, here, :] = one if ref is v_ref else _turn(one.astype(F32), c, s).astype(BF)

        lax.fori_loop(0, TOKENS // B, project, None)
        for r in range(4):
            weights.close(last, r)
        sums = TpReduce(at, *reduce)

        def tile(n, _):
            t = sums.block(n)
            here = _block(t)
            top_s[:] = jnp.full_like(top_s, NEG)
            mix_s[:] = jnp.zeros_like(mix_s)
            ones = jnp.ones((8, B), BF)

            @pl.when(n == 0)
            def _():
                weights.next(down, 1)
                other.launch(1, 0)

            @pl.when(n == 1)
            def _():
                states[1].middle()
                weights.next(gate, 1)
                other.launch(0, 1)

            @pl.when(n == 2)
            def _():
                weights.next(down, 2)
                other.launch(1, 1)

            @pl.when(n == 3)
            def _():
                weights.next(gate, 2)
                other.launch(0, 2)
                weights.launch(up, 0)

            def block(j, masked):
                keys = _block(j)
                scores = [_mt(k_ref[h, keys, :], q_ref[h, here, :]) for h in range(HEADS)]
                weigh, keep = [], []
                for h, sc in enumerate(scores):
                    if masked:
                        sc = jnp.where(gap_s[:] >= 0, sc, HIDDEN)
                    one = slice(h, h + 1)
                    old = top_s[one, :]
                    top = jnp.maximum(old, sc.max(axis=0, keepdims=True))
                    top_s[one, :] = top
                    weigh.append(jnp.exp2((sc - top) * e).astype(BF))
                    keep.append(jnp.exp2((old - top) * e))
                for h in range(HEADS):
                    values = jnp.concatenate([v_ref[h, keys, :].T, ones], axis=0)
                    mix_s[h] = mix_s[h] * keep[h] + _mm(values, weigh[h])

            lax.fori_loop(0, t, lambda j, _: block(j, False), None)
            block(t, True)
            for h in range(HEADS):
                one = slice(h, h + 1)
                total = mix_s[h, HEAD : HEAD + 1, :]
                o_ref[h, here, :] = (mix_s[h, :HEAD, :] * (1 / total)).T.astype(BF)
                lse_ref[one, here] = top_s[one, :] * SCALE + jnp.log(total)

            mixed = jnp.concatenate([o_ref[h, here, :] for h in range(HEADS)], axis=1)
            sums.add(n, _mm(mixed, wo_s[:].reshape(B, B)))

        lax.fori_loop(0, TOKENS // B, tile, None)
        weights.next(down, 3)
        other.launch(1, 2)
        weights.next(gate, 3)
        keep = ((q_ref, q_out), (k_ref, k_out), (v_ref, v_out), (o_ref, o_out), (a_s, a_out), (wqkv_s, wqkv_out), (wo_s, wo_out))
        keep = [pltpu.make_async_copy(s, o, ls.at[n]) for n, (s, o) in enumerate(keep)]
        for c in keep:
            c.start()
        h = (x_ref[:].astype(F32) + _round(sums.total())).astype(BF)
        h_ref[:] = h
        b_s[:] = _normed(h.astype(F32)).astype(BF)
        states[2].start()
        for r in range(1, 4):
            weights.next(up, r)
        states[2].middle()
        states[1].finish()
        states[2].finish()
        for n in (down, gate, up):
            for r in range(4):
                weights.close(n, r)
        other.close()
        for c in keep:
            c.wait()

    wqkv, last = (8, 3, *wq.shape), (8, *wo.shape)
    outs = [BLOCK, STATES, STATES, STATES, _shape(wqkv), _shape(last), *[_shape((8, *w.shape)) for w in (wg, wu, wd)], *[PER_HEAD] * 4,
            _shape((HEADS, TOKENS), F32), *[_shape((TOKENS, HEAD), F32)] * 2]
    scratch = [pltpu.VMEM((4, B, B), BF), pltpu.VMEM((B, B), BF), pltpu.VMEM(wqkv, BF), pltpu.VMEM(last, BF), *[pltpu.VMEM(PER_HEAD.shape, BF)] * 4,
               pltpu.VMEM((HEADS, B), F32), pltpu.VMEM((HEADS, HEAD + 8, B), F32), pltpu.VMEM((B, B), jnp.int32),
               *_sems((3, 3), (3, 3), (3,), (5, MOVES), (5, MOVES), (5,), (MOVES,), (MOVES,), (), (7,)), *_tp_scratch()]
    return _comm(kernel, "forward", 0, (x, dy, wq, wk, wv, wo, wg, wu, wd), outs, [INV] + [ANY] * 12 + [INV] * 3, scratch, [INV] * 9)


def _ffn(b, dy, g, u, d, h):
    chunks, per = FF // WIDE, WIDE // 256

    def kernel(b_any, dy_any, g_ref, u_ref, d_ref, h_ref, dh_ref, dh_out, dg_out, du_out, dd_out, early_out,
               b_ref, dy_ref, g_s, u_s, d_s, dgate_s, dup_s, hidden_s, bt_s, dyt_s, wdt_s, wgut_s, db_s, ls, gs, gr, gl, ys, yr, *reduce):
        at = Place()
        loads = [pltpu.make_async_copy(s, o, ls.at[n]) for n, (s, o) in enumerate(((g_ref, g_s), (u_ref, u_s), (d_ref, d_s), (b_any, b_ref), (dy_any, dy_ref)))]
        for c in loads:
            c.start()
        at.meet(True, True)
        for c in loads:
            c.wait()
        sums = TpReduce(at, *reduce)

        def columns(j):
            return pl.ds(j * WIDE, WIDE) if isinstance(j, int) else pl.ds(pl.multiple_of(j * WIDE, WIDE), WIDE)

        def prepare(j, _):
            c = columns(j)
            wdt_s[:, c] = d_s[pl.ds(j * per, per)].reshape(WIDE, B).T
            wgut_s[j, :WIDE] = g_s[:, :, c].reshape(B, WIDE).T
            wgut_s[j, WIDE:] = u_s[:, :, c].reshape(B, WIDE).T

        lax.fori_loop(0, chunks, prepare, None)

        def tile(k, _):
            t = sums.block(k)
            rows = _block(t)
            b, dy = b_ref[t], dy_ref[t]
            bt_s[:, rows] = b.T
            dyt_s[:, rows] = dy.T
            db_s[:] = jnp.zeros_like(db_s)

            def hidden(j):
                c = columns(j)
                gate = _mm(b, g_s[:, :, c].reshape(B, WIDE))
                up = _mm(b, u_s[:, :, c].reshape(B, WIDE))
                dh = _round(_mm(dy, wdt_s[:, c]))
                sig = jax.nn.sigmoid(gate)
                act = gate * sig
                dup = (dh * act).astype(BF)
                dgate = (dh * up * (sig + act * (1 - sig))).astype(BF)
                hidden_s[rows, c] = (act * up).astype(BF)
                dup_s[rows, c] = dup
                dgate_s[rows, c] = dgate

            def states(j):
                c = columns(j)
                db_s[:] += _mm(jnp.concatenate([dgate_s[rows, c], dup_s[rows, c]], axis=1), wgut_s[j])

            hidden(0)
            for j in range(1, chunks):
                hidden(j)
                states(j - 1)
            states(chunks - 1)
            sums.add(k, db_s[:])

        lax.fori_loop(0, TOKENS // B, tile, None)
        back = _normed_bwd(h_ref[:].astype(F32), _round(sums.total()))
        dh_ref[:] = (dy_ref[at.tp].astype(F32) + _round(back)).astype(BF)
        states = TpGather(at, dh_ref, dh_out, gs, gr, gl)
        states.start()

        def down(i, _):
            j = lax.rem(i + lax.div(at.other_row, 2), 4)
            d_s[pl.ds(2 * j, 2)] = _mm(dyt_s[:], hidden_s[:, _block(j)]).T.astype(BF).reshape(2, B // 2, B)

        lax.fori_loop(0, 2, down, None)
        stores = [pltpu.make_async_copy(s, o, ls.at[n]) for n, (s, o) in enumerate(((g_s, dg_out), (u_s, du_out), (d_s, dd_out)))]

        def across(z):
            return [_send(d_s.at[at.other_row + d], early_out.at[d], ys.at[i], yr.at[i], at.to_y) for i, d in enumerate(ORDER[z][:EARLY])]

        for z in range(4):

            @pl.when(at.z == z)
            def _():
                for c in across(z):
                    c.start()

        lax.fori_loop(2, 4, down, None)
        stores[2].start()
        for term, out in ((dgate_s, g_s), (dup_s, u_s)):

            def gate_up(j, _):
                out[:, :, _block(j)] = _mm(bt_s[:], term[:, _block(j)]).astype(BF).reshape(8, B // 8, B)

            lax.fori_loop(0, FF // B, gate_up, None)
            if out is g_s:
                stores[0].start()
                states.middle()
        stores[1].start()
        states.finish()
        for z in range(4):

            @pl.when(at.z == z)
            def _():
                for c in across(z):
                    c.wait()

        for c in stores:
            c.wait()

    wide, tall, big = pltpu.VMEM((B, FF), BF), pltpu.VMEM(g.shape, BF), pltpu.VMEM((TOKENS, FF), BF)
    scratch = [pltpu.VMEM(b.shape, BF), pltpu.VMEM(b.shape, BF), tall, tall, pltpu.VMEM(d.shape, BF), big, big, big, wide, wide, wide, pltpu.VMEM((chunks, 2 * WIDE, B), BF), pltpu.VMEM((B, B), F32),
               *_sems((5,), (3,), (3,), (), (EARLY,), (EARLY,)), *_tp_scratch()]
    outs = [BLOCK, STATES, _shape(g.shape), _shape(u.shape), _shape(d.shape), _shape((4, *d.shape[1:]))]
    return _comm(kernel, "ffn", 3, (b, dy, g, u, d, h), outs, [INV] + [ANY] * 5, scratch, [ANY] * 5 + [INV])


def _back(dh, a, wqkv, wo, cos, sin, q, k, v, heads, lse, early, parts):
    e = SCALE * LOG2E
    count = len(parts)

    def kernel(*refs):
        given, (early_ref, *refs) = refs[: len(held)], refs[len(held) :]
        parts_ref, (da_ref, dwq_ref, dwk_ref, dwv_ref, dwo_out, early_out, *refs) = refs[:count], refs[count:]
        outs, (hs, dwo_s, ws, wr, wl, *refs) = refs[:count], refs[count:]
        here, (do_s, dq_s, dk_s, dv_s, gap_s, acc_s, *refs) = refs[: len(held)], refs[len(held) :]
        dh_s, a_ref, wqkv_ref, wo_ref, cos_ref, sin_ref, q_ref, k_ref, v_ref, o_ref, lse_ref = here
        loads = [pltpu.make_async_copy(s, o, hs.at[n]) for n, (s, o) in enumerate(zip(given, here))]
        scratch, (ds, dr, dl) = refs[: 4 * count], refs[4 * count :]
        at = Place()
        at.meet(True, False)
        sums = DpReduce(at, parts_ref, [scratch[4 * n : 4 * n + 4] for n in range(count)], ds, dr, dl, early_ref, EARLY)
        sums.start()
        for c in loads:
            c.start()
        gap_s[:] = _gap((B, B))
        acc_s[:] = jnp.zeros_like(acc_s)
        dk_s[:] = jnp.zeros_like(dk_s)
        dv_s[:] = jnp.zeros_like(dv_s)
        sums.ready()
        sums.stage(0, 0)
        for c in loads:
            c.wait()
        mixed = [jnp.concatenate([o_ref[h, _block(t), :] for h in range(HEADS)], axis=1) for t in range(4)]
        dwo_s[:] = sum(_tm(m, dh_s[t]) for t, m in enumerate(mixed)).astype(BF).reshape(dwo_s.shape)
        mix_store = pltpu.make_async_copy(dwo_s, dwo_out, wl)
        mix_store.start()
        mix_sends = [_send(dwo_s.at[at.other_row + d], early_out.at[d], ws.at[d], wr.at[d], at.to_y) for d in range(4)]
        for c in mix_sends:
            c.start()

        def tile(i, _):
            t = 3 - i
            here = _block(t)


            @pl.when(i == 1)
            def _():
                sums.stage(0, 2)
                sums.stage(1, 1)

            pl.when(i == 2)(lambda: sums.stage(1, 2))
            pl.when(i == 3)(lambda: sums.stage(2, 2))
            dh = dh_s[t]
            mixed = [o_ref[h, here, :] for h in range(HEADS)]
            do_s[:] = _mt(dh, wo_ref[:].reshape(B, B)).astype(BF)
            dos = _heads(do_s)
            deltas = [(x.astype(F32) * y.astype(F32)).T.sum(axis=0, keepdims=True) for x, y in zip(dos, mixed)]
            lses = [lse_ref[h : h + 1, here] * LOG2E for h in range(HEADS)]
            dq_s[:] = jnp.zeros_like(dq_s)

            def block(j, masked):
                keys = _block(j)
                scores = [_mt(k_ref[h, keys, :], q_ref[h, here, :]) for h in range(HEADS)]
                dps = [_mt(v_ref[h, keys, :], do_s[:, h * HEAD : (h + 1) * HEAD]) for h in range(HEADS)]
                for h in range(HEADS):
                    p = jnp.exp2(scores[h] * e - lses[h])
                    if masked:
                        p = jnp.where(gap_s[:] >= 0, p, 0.0)
                    ds = (p * (dps[h] - deltas[h])).astype(BF)
                    dv_s[h, keys, :] += _mm(p.astype(BF), do_s[:, h * HEAD : (h + 1) * HEAD])
                    dk_s[h, keys, :] += _mm(ds, q_ref[h, here, :])
                    dq_s[h] += _mm(k_ref[h, keys, :].T, ds)

            def whole(j, _):
                @pl.when(jnp.logical_and(i == 0, j == 1))
                def _():
                    sums.stage(0, 1)
                    sums.stage(1, 0)

                pl.when(jnp.logical_and(i == 0, j == 2))(lambda: sums.stage(2, 0))
                pl.when(jnp.logical_and(i == 1, j == 1))(lambda: sums.stage(2, 1))
                block(j, False)

            lax.fori_loop(0, t, whole, None)
            block(t, True)
            c, s = cos_ref[here, :], -sin_ref[here, :]
            da = jnp.zeros((B, B), F32)
            for n, ref in enumerate((dq_s, dk_s, dv_s)):
                g = []
                for h in range(HEADS):
                    one = dq_s[h].T if ref is dq_s else ref[h, here, :]
                    g.append(one.astype(BF) if ref is dv_s else _turn(_round(one * SCALE), c, s).astype(BF))
                g = jnp.concatenate(g, axis=1)
                da += _mt(g, wqkv_ref[:, n].reshape(B, B))
                acc_s[n] += _tm(a_ref[t], g)
            da_ref[t] = da.astype(BF)

        lax.fori_loop(0, TOKENS // B, tile, None)
        for n, ref in enumerate((dwq_ref, dwk_ref, dwv_ref)):
            ref[:] = acc_s[n].astype(BF)
        sums.finish(outs)
        mix_store.wait()
        for c in mix_sends:
            c.wait()

    held = (dh, a, wqkv, wo, cos, sin, q, k, v, heads, lse)
    blocks = [p.shape[1:] for p in parts]
    scratch = [*_sems((len(held),)), pltpu.VMEM(wo.shape, BF), *_sems((4,), (4,), ()), *[pltpu.VMEM(t.shape, t.dtype) for t in held], pltpu.VMEM((B, B), BF), pltpu.VMEM((HEADS, HEAD, B), F32), pltpu.VMEM(PER_HEAD.shape, F32), pltpu.VMEM(PER_HEAD.shape, F32),
               pltpu.VMEM((B, B), jnp.int32), pltpu.VMEM((3, B, B), F32), *_reduce_scratch(blocks), *_reduce_sems(count)]
    return _comm(kernel, "back", 4, (*held, early, *parts), [STATES, *[BLOCK] * 3, _shape(wo.shape), _shape((4, *wo.shape[1:])), *map(_shape, blocks)], [INV] * 4 + [ANY] * 2 + [INV] * count, scratch,
                 [ANY] * (len(held) + 1 + count))


def _finish(da, x, dh, early, parts):
    count = len(parts)

    def kernel(da_ref, x_ref, dh_ref, early_ref, *refs):
        parts_ref, (dx_ref, *refs) = refs[:count], refs[count:]
        outs, (*refs, ds, dr, dl) = refs[:count], refs[count:]
        tp = len(refs) - 4 * count
        reduce, scratch = refs[:tp], refs[tp:]
        at = Place()
        at.meet(True, True)
        weights = DpReduce(at, parts_ref, [scratch[4 * n : 4 * n + 4] for n in range(count)], ds, dr, dl, early_ref, 4)
        weights.start()
        weights.ready()
        weights.stage(0, 0)
        sums = TpReduce(at, *reduce)
        for k in range(4):
            sums.add(k, da_ref[sums.block(k)].astype(F32))
        for s in range(3):
            for n in range(count):
                if s + n > 0:
                    weights.stage(n, s)
        back = _normed_bwd(x_ref[:].astype(F32), _round(sums.total()))
        dx_ref[:] = (dh_ref[:].astype(F32) + _round(back)).astype(BF)
        weights.finish(outs)

    blocks = [p.shape[1:] for p in parts]
    scratch = [*_tp_scratch(), *_reduce_scratch(blocks), *_reduce_sems(count)]
    return _comm(kernel, "finish", 5, (da, x, dh, early, *parts), [BLOCK, *map(_shape, blocks)], [INV] * (1 + count), scratch, [INV] * 3 + [ANY] * (1 + count))


def _copies(arrays):
    count = len(arrays)

    def kernel(*refs):
        for a, b in zip(refs[:count], refs[count:]):
            b[:] = a[:]

    return pl.pallas_call(kernel, name="copies", out_shape=[_shape(a.shape) for a in arrays], in_specs=[INV] * count, out_specs=[INV] * count)(*arrays)


def solution(mesh):
    def step(x, dy, wq, wk, wv, wo, wg, wu, wd):
        x, dy = x[0], dy[0]
        h, b, a, all_dy, wqkv, wo, g, u, d, q, k, v, heads, lse, cos, sin = _forward(x, dy, wq, wk, wv, wo, wg, wu, wd)
        dh, all_dh, dg, du, dd, early = _ffn(b, all_dy, g, u, d, h)
        da, dwq, dwk, dwv, dwo, early, *more = _back(all_dh, a, wqkv, wo, cos, sin, q, k, v, heads, lse, early, (dd, dg, du))
        parts = [dwo, *[w.reshape(wo.shape) for w in (dwq, dwk, dwv)]]
        dx, dwo, dwq, dwk, dwv, dd, dg, du = _copies([*_finish(da, x, dh, early, parts), *more])
        return dx[None], dwq, dwk, dwv, dwo, dg, du, dd

    states, by_columns, by_rows = P("dp", "tp", None), P("dp", "tp"), P(("tp", "dp"), None)
    weights = (by_columns, by_columns, by_columns, by_rows, by_columns, by_columns, by_rows)
    return jax.shard_map(step, mesh=mesh, in_specs=(states, states, *weights), out_specs=(states, *weights), check_vma=False)
```
